32 devices in a mesh: grp: 4 (over y, x), dom: 8 (over z, core).
Axes of the slice: x: 2, y: 2, z: 4, core: 2. Of those that a mesh axis runs over, the one named last changes fastest.
Arguments:
- node_state: float32 [4096, 6, 128], P(('grp', 'dom')), may hold values from -6 to 6
- node_dest: int32 [4096], P(('grp', 'dom')), may hold values from 0 to 7, as said below
- seg_nodes: float32 [6, 16384], P(None, ('grp', 'dom')), may hold values from -6 to 6
- seg_conn: int32 [3, 32768], P(None, ('grp', 'dom')), may hold values from 0 to 511
- pair_seg: int32 [32, 4, 32], P(('grp', 'dom')), may hold values from 0 to 7
- pair_slot: int32 [32, 4, 32], P(('grp', 'dom')), may hold values from 0 to 255, as said below
Outputs:
- node_force: float32 [4096, 3, 128], P(('grp', 'dom'))
The draws below stay inside these ranges and needn't reach their ends.
Inputs may be any that keep to these rules, and one draw needn't show every extreme that they name: `node_dest`: at most 32 blocks of one device name the same contact domain; in every grp row one contact domain receives exactly 32 blocks from every device of that row; every device sends at least one block to the contact domain of its own dom index. `pair_slot`: every entry names a slot d * 32 + k that holds a block: device (r, d) sends more than k blocks to the contact domain.
All inputs are finite; a program needn't handle non-finite values.
Results may differ from the reference program's by a relative error of at most 0.00023.
Values sent between devices are 32-bit elements; how exact they have to be, the bound alone decides.
A program may use at most 64 MiB of HBM per device.

```python
import jax
import jax.numpy as jnp
from jax import lax

NODE_BLK = 128
SEG_BLK = 128
NB_DEV = 128
SB_DEV = 8
PAIR_GRP = 32
SN_DEV = 512
CAP = 32
ALL_BLK = 4096
ALL_SEG = 32768
ALL_SN = 16384
N_GRP = 4
N_DOM = 8


def route_tables(key):
    base = jax.random.fold_in(key, 4242)
    key_perm, key_hot, key_shuffle, key_pick = jax.random.split(base, 4)
    senders = N_GRP * N_DOM
    tokens = N_DOM * CAP
    hot_dom = jax.random.randint(key_hot, (N_GRP,), 0, N_DOM)
    perms = jax.vmap(lambda sub_key: jax.random.permutation(sub_key, tokens))(jax.random.split(key_perm, senders))
    sender_ids = jnp.arange(senders, dtype=jnp.int32)
    row_ids = sender_ids // N_DOM
    own_dom = sender_ids % N_DOM
    token_dom = perms // CAP
    is_hot = token_dom == hot_dom[row_ids][:, None]
    is_own = (token_dom == own_dom[:, None]) & (perms % CAP == 0) & jnp.logical_not(is_hot)
    priority = jnp.where(is_hot, 0, jnp.where(is_own, 1, 2))
    score = priority * tokens + jnp.arange(tokens, dtype=jnp.int32)[None, :]
    order_ids = jnp.argsort(score, axis=1)
    chosen = jnp.take_along_axis(perms, order_ids, axis=1)[:, :NB_DEV] // CAP
    shuffles = jax.vmap(lambda sub_key: jax.random.permutation(sub_key, NB_DEV))(jax.random.split(key_shuffle, senders))
    target_dom = jnp.take_along_axis(chosen, shuffles, axis=1).astype(jnp.int32)
    counts = jnp.sum((target_dom[:, :, None] == jnp.arange(N_DOM, dtype=jnp.int32)[None, None, :]).astype(jnp.int32), axis=1)
    per_row = counts.reshape(N_GRP, N_DOM, N_DOM)
    live = jnp.arange(CAP, dtype=jnp.int32)[None, None, None, :] < per_row[:, :, :, None]
    live = jnp.transpose(live, (0, 2, 1, 3)).reshape(N_GRP, N_DOM, N_DOM * CAP).astype(jnp.int32)
    running = jnp.cumsum(live, axis=2)
    total_live = running[:, :, -1]
    raw_pick = jax.random.randint(key_pick, (N_GRP, N_DOM, N_GRP, PAIR_GRP), 0, 1 << 30)
    limit = jnp.transpose(total_live, (1, 0))
    chosen_rank = raw_pick % limit[None, :, :, None]
    run_table = jnp.transpose(running, (1, 0, 2))
    slot_ids = jnp.sum((run_table[None, :, :, None, :] <= chosen_rank[..., None]).astype(jnp.int32), axis=-1)
    return (target_dom.reshape(-1), slot_ids.reshape(N_GRP * N_DOM, N_GRP, PAIR_GRP).astype(jnp.int32))


def draw_node_dest(key, part):
    return route_tables(key)[0]


def draw_pair_slot(key, part):
    return route_tables(key)[1]


def with_ends(drawn, stream_key, smallest, largest):
    dims = drawn.shape
    index_at = [jax.random.randint(jax.random.fold_in(stream_key, axis), (), 0, dims[axis]) for axis in range(len(dims))]
    drawn = drawn.at[tuple(index_at)].set(smallest)
    longest = dims.index(max(dims))
    index_at[longest] = (index_at[longest] + 1) % dims[longest]
    return drawn.at[tuple(index_at)].set(largest)


def level_of(stream_key, shape, pieces, smallest, largest):
    def one(dim, blocks):
        steps = jax.random.uniform(jax.random.fold_in(jax.random.fold_in(stream_key, 6), dim), (blocks,), jnp.float32, smallest / len(pieces), largest / len(pieces))
        return jnp.repeat(jnp.exp(steps), shape[dim] // blocks).reshape((-1,) + (1,) * (len(shape) - dim - 1))

    level = one(*pieces[0])
    for cut in pieces[1:]:
        level = level * one(*cut)
    return level


def normal_values(own_key, dims, scale, most, cuts=(), kind=jnp.bfloat16):
    values = jax.random.normal(own_key, dims, jnp.float32) * scale
    if len(cuts) > 0:
        values = level_of(own_key, dims, cuts, -0.22, 0.18) * values
    return jnp.clip(values, min=-most, max=most).astype(kind)


def setup_inputs(seed: int = 0) -> dict:
    arg_keys = jax.random.split(jax.random.key(seed), 7)
    node_state = normal_values(arg_keys[0], (ALL_BLK, 6, NODE_BLK), 1.0, 6.0, ((0, 32),), jnp.float32)
    node_dest = draw_node_dest(jax.random.fold_in(arg_keys[6], 71), 0)
    seg_nodes = normal_values(arg_keys[2], (6, ALL_SN), 1.0, 6.0, ((1, 32),), jnp.float32)
    seg_conn = with_ends(jax.random.randint(arg_keys[3], (3, ALL_SEG), 0, SN_DEV), jax.random.fold_in(arg_keys[3], 1), 0, SN_DEV - 1).astype(jnp.int32)
    pair_seg = with_ends(jax.random.randint(arg_keys[4], (N_GRP * N_DOM, N_GRP, PAIR_GRP), 0, SB_DEV), jax.random.fold_in(arg_keys[4], 1), 0, SB_DEV - 1).astype(jnp.int32)
    pair_slot = draw_pair_slot(jax.random.fold_in(arg_keys[6], 71), 0)
    return dict(node_state=node_state, node_dest=node_dest, seg_nodes=seg_nodes, seg_conn=seg_conn, pair_seg=pair_seg, pair_slot=pair_slot)


time_step = 0.5
stiffness = 0.5
radius_sq = 0.5


def seg_geometry(corners):
    corner_a = corners[:, 0]
    corner_b = corners[:, 1]
    corner_c = corners[:, 2]
    edge_one = corner_b[0:3] - corner_a[0:3]
    edge_two = corner_c[0:3] - corner_a[0:3]
    normal = 0.5 * jnp.stack([
        edge_one[1] * edge_two[2] - edge_one[2] * edge_two[1],
        edge_one[2] * edge_two[0] - edge_one[0] * edge_two[2],
        edge_one[0] * edge_two[1] - edge_one[1] * edge_two[0]])
    centre = (corner_a[0:3] + corner_b[0:3] + corner_c[0:3]) / 3.0
    motion = (corner_a[3:6] + corner_b[3:6] + corner_c[3:6]) / 3.0
    return jnp.concatenate([normal, centre, motion], axis=0)


def tile_force(node_rows, geometry):
    clearance = jnp.zeros((geometry.shape[1], node_rows.shape[1]), jnp.float32)
    distance = jnp.zeros((geometry.shape[1], node_rows.shape[1]), jnp.float32)
    for axis_id in range(3):
        offset = node_rows[axis_id][None, :] - geometry[3 + axis_id][:, None]
        drift = node_rows[3 + axis_id][None, :] - geometry[6 + axis_id][:, None]
        clearance = clearance + geometry[axis_id][:, None] * (offset + time_step * drift)
        distance = distance + offset * offset
    pressure = stiffness * jnp.exp(-distance / radius_sq) * jnp.maximum(-clearance, 0.0)
    return jnp.dot(geometry[0:3], pressure, precision=lax.Precision.HIGHEST, preferred_element_type=jnp.float32)


def reference(node_state, node_dest, seg_nodes, seg_conn, pair_seg, pair_slot):
    devices = N_GRP * N_DOM
    seg_owner = jnp.arange(seg_conn.shape[1], dtype=jnp.int32) // (SB_DEV * SEG_BLK)
    corners = jnp.take(seg_nodes, seg_conn + (seg_owner * SN_DEV)[None, :], axis=1)
    geometry = seg_geometry(corners)
    geo_blocks = jnp.transpose(geometry.reshape(9, devices * SB_DEV, SEG_BLK), (1, 0, 2))
    target_dom = node_dest.reshape(devices, NB_DEV)
    order_ids = jnp.arange(NB_DEV, dtype=jnp.int32)
    earlier = order_ids[None, :] < order_ids[:, None]
    same_dom = target_dom[:, :, None] == target_dom[:, None, :]
    slot_rank = jnp.sum((same_dom & earlier[None, :, :]).astype(jnp.int32), axis=2)
    device_ids = jnp.arange(devices, dtype=jnp.int32)
    contact_dom = (device_ids % N_DOM)[:, None, None]
    sender = jnp.arange(N_GRP, dtype=jnp.int32)[None, :, None] * N_DOM + pair_slot // CAP
    wanted_rank = pair_slot % CAP
    matching = (target_dom[sender] == contact_dom[..., None]) & (slot_rank[sender] == wanted_rank[..., None])
    local_block = jnp.sum(jnp.where(matching, order_ids, 0), axis=3)
    block_ids = (sender * NB_DEV + local_block).astype(jnp.int32)
    seg_ids = (device_ids[:, None, None] * SB_DEV + pair_seg).astype(jnp.int32)

    def device_forces(device_idx):
        node_rows = jnp.take(node_state, block_ids[device_idx].reshape(-1), axis=0)
        seg_rows = jnp.take(geo_blocks, seg_ids[device_idx].reshape(-1), axis=0)
        return jax.vmap(tile_force)(node_rows, seg_rows)

    forces = lax.map(device_forces, device_ids)
    return jax.ops.segment_sum(forces.reshape(-1, 3, NODE_BLK), block_ids.reshape(-1), num_segments=devices * NB_DEV)
```

```python
import functools
import math

import jax
import jax.numpy as jnp
from jax import lax
from jax.experimental import pallas as pl
from jax.experimental.pallas import tpu as pltpu
from jax.sharding import PartitionSpec as P

BLK = 128
time_step = 0.5
stiffness = 0.5
radius_sq = 0.5
ALPHA = -math.log2(math.e) / radius_sq
F32 = jnp.float32
BF16 = jnp.bfloat16
VMEM = pl.BlockSpec(memory_space=pltpu.VMEM)
UNROLL = 4


def iota(shape, axis):
    return lax.broadcasted_iota(jnp.int32, shape, axis)


def write_geometry(seg_nodes, seg_conn, store):
    blocks = seg_conn.shape[1] // BLK
    tiles = seg_nodes.shape[1] // BLK
    corners = []
    for corner in range(3):
        index = jnp.concatenate(
            [seg_conn[corner : corner + 1, b * BLK : (b + 1) * BLK] for b in range(blocks)], axis=0
        )
        tile_id = index // BLK
        lane = index % BLK
        rows = []
        for row in range(6):
            value = None
            for t in range(tiles):
                table = jnp.broadcast_to(
                    seg_nodes[row : row + 1, t * BLK : (t + 1) * BLK], (blocks, BLK)
                )
                picked = jnp.take_along_axis(table, lane, axis=1)
                value = picked if value is None else jnp.where(tile_id == t, picked, value)
            rows.append(value)
        corners.append(rows)
    a, b, c = corners
    one = [b[i] - a[i] for i in range(3)]
    two = [c[i] - a[i] for i in range(3)]
    normal = [
        0.5 * (one[1] * two[2] - one[2] * two[1]),
        0.5 * (one[2] * two[0] - one[0] * two[2]),
        0.5 * (one[0] * two[1] - one[1] * two[0]),
    ]
    mean = [(a[i] + b[i] + c[i]) / 3.0 for i in range(6)]
    norm = mean[0] * mean[0] + mean[1] * mean[1] + mean[2] * mean[2]
    shift = sum(normal[i] * (mean[i] + time_step * mean[3 + i]) for i in range(3))
    for i in range(3):
        store(i, (-2.0 * ALPHA) * mean[i])
        store(4 + i, -stiffness * normal[i])
    store(3, ALPHA * norm)
    store(7, stiffness * shift)


def geometry_kernel(nodes_ref, conn_ref, seg_ref, slot_ref, out_ref):
    blocks = conn_ref.shape[1] // BLK
    groups = seg_ref.shape[1]

    def store(row, value):
        out_ref[0:blocks, row, :] = value

    write_geometry(nodes_ref[...], conn_ref[...], store)
    for row, ref in ((0, seg_ref), (1, slot_ref)):
        flat = jnp.concatenate([ref[0, r : r + 1, :] for r in range(groups)], axis=1)
        out_ref[blocks, row : row + 1, :] = flat.astype(F32)
    out_ref[blocks, 2:8, :] = jnp.zeros((6, BLK), F32)


def pack_lanes(value, rows):
    return jnp.concatenate(
        [value[i * rows : (i + 1) * rows] for i in range(value.shape[0] // rows)], axis=1
    )


def pair_list(seg, slot, dest, my_dom, dom_count, seg_blocks, capacity, width):
    rows = seg.shape[0]
    nb = dest.shape[1]
    spread = jnp.broadcast_to(dest.astype(F32), (nb, nb))
    column = spread.T
    lower = iota((nb, nb), 1) < iota((nb, nb), 0)
    rank = jnp.sum(jnp.where((spread == column) & lower, 1.0, 0.0), axis=1, keepdims=True)
    own_key = column * float(capacity) + rank

    source = (iota((rows, BLK), 1) // width) * rows + iota((rows, BLK), 0)
    mine = slot // capacity == my_dom
    key = ((source % dom_count) * capacity + slot % capacity).astype(F32)
    block = source * seg_blocks + seg
    mask = jnp.where(mine, 1.0, 0.0)
    strict = jnp.where(iota((BLK, BLK), 0) < iota((BLK, BLK), 1), 1.0, 0.0)
    before = jnp.dot(mask.astype(BF16), strict.astype(BF16), preferred_element_type=F32)
    above = jnp.where(iota((rows, rows), 1) < iota((rows, rows), 0), 1.0, 0.0)
    ahead = jnp.sum(
        jnp.dot(above.astype(BF16), mask.astype(BF16), preferred_element_type=F32),
        axis=1,
        keepdims=True,
    )
    position = (before + ahead).astype(jnp.int32)
    count = jnp.sum(mask)
    high = jnp.where(mine, position // BLK, -1)
    low = position % BLK
    node_iota = iota((nb, BLK), 0).astype(F32)
    total = jnp.zeros((3 * rows, BLK), F32)
    for row in range(rows):
        cut = slice(row, row + 1)
        node = jnp.sum(jnp.where(own_key == key[cut], node_iota, 0.0), axis=0, keepdims=True)
        hot = jnp.where(iota((BLK, BLK), 0) == low[cut], 1.0, 0.0).astype(BF16)
        here = iota((rows, BLK), 0) == high[cut]
        codes = [node, (block[cut] % 256).astype(F32), (block[cut] // 256).astype(F32)]
        lhs = jnp.concatenate([jnp.where(here, code, 0.0) for code in codes], axis=0)
        total = total + lax.dot_general(
            lhs.astype(BF16), hot, (((1,), (1,)), ((), ())), preferred_element_type=F32
        )
    total = total.astype(jnp.int32)
    return total[0:rows], total[rows : 2 * rows] + 256 * total[2 * rows : 3 * rows], count


def split3(value):
    hi = value.astype(BF16).astype(F32)
    rest = value - hi
    mid = rest.astype(BF16).astype(F32)
    return hi, mid, rest - mid


def node_side(node):
    place = node[0:3]
    ahead = place + time_step * node[3:6]
    ones = jnp.ones((1, BLK), F32)
    zeros = jnp.zeros((4, BLK), F32)
    square = split3(ALPHA * jnp.sum(place * place, axis=0, keepdims=True))
    pad = jnp.zeros((13, BLK), F32)
    eh, em, el = split3(jnp.concatenate([place, ones, zeros], axis=0))
    ch, cm, cl = split3(jnp.concatenate([zeros, ahead, ones], axis=0))
    left = jnp.concatenate([eh, em, el, eh, em, eh, *square, pad], axis=0)
    right = jnp.concatenate([ch, cm, cl, ch, cm, ch, jnp.zeros((16, BLK), F32)], axis=0)
    return jnp.concatenate([left.astype(BF16), right.astype(BF16)], axis=1)


def pair_force(geo, node):
    hi, mid, lo = split3(geo)
    ones = jnp.ones((16, BLK), F32)
    left = jnp.concatenate([hi, hi, hi, mid, mid, lo, ones], axis=0).astype(BF16)
    both = lax.dot_general(
        left, node_side(node), (((0,), (0,)), ((), ())), preferred_element_type=F32
    )
    pressure = jnp.exp2(both[:, 0:BLK]) * jnp.maximum(both[:, BLK:], 0.0)
    top = pressure.astype(BF16)
    bottom = (pressure - top.astype(F32)).astype(BF16)
    weights = jnp.concatenate([hi, mid], axis=0).astype(BF16)
    result = jnp.dot(
        jnp.concatenate([weights, weights], axis=1),
        jnp.concatenate([top, bottom], axis=0),
        preferred_element_type=F32,
    )
    return result[0:8] + result[8:16]


def force_kernel(
    dom_count, capacity, width, geo_ref, node_ref, dest_ref, out_ref, list_vmem, list_smem, acc_ref, sem
):
    my_dom = lax.axis_index("dom")
    my_row = lax.axis_index("grp")
    devices, planes = geo_ref.shape[0], geo_ref.shape[1]
    seg_blocks = planes - 1
    rows = devices * width // BLK
    tables = []
    for row in range(2):
        full = geo_ref[:, seg_blocks, row, :]
        value = None
        for r in range(BLK // width):
            piece = full[:, r * width : (r + 1) * width]
            value = piece if value is None else jnp.where(my_row == r, piece, value)
        tables.append(pack_lanes(value, rows).astype(jnp.int32))
    nodes, blocks, count = pair_list(
        tables[0], tables[1], dest_ref[...], my_dom, dom_count, seg_blocks, capacity, width
    )
    list_vmem[0:rows] = nodes
    list_vmem[rows : 2 * rows] = blocks
    list_vmem[2 * rows : 2 * rows + 1] = jnp.full((1, BLK), count, F32).astype(jnp.int32)
    copy = pltpu.make_async_copy(list_vmem, list_smem, sem)
    copy.start()
    acc_ref[...] = jnp.zeros_like(acc_ref)
    copy.wait()
    pairs = list_smem[2 * rows, 0]

    def body(step, carry):
        results = []
        for u in range(UNROLL):
            p = jnp.minimum(step * UNROLL + u, rows * BLK - 1)
            node_id = list_smem[p // BLK, p % BLK]
            block_id = list_smem[rows + p // BLK, p % BLK]
            geo = geo_ref[block_id // seg_blocks, block_id % seg_blocks]
            results.append((p, node_id, pair_force(geo, node_ref[:, node_id, :])))
        for u in range(UNROLL):
            p, node_id, force = results[u]
            scale = jnp.where(step * UNROLL + u < pairs, -1.0 / stiffness, 0.0)
            acc_ref[node_id] = acc_ref[node_id] + scale * force
        return carry

    lax.fori_loop(0, (pairs + UNROLL - 1) // UNROLL, body, 0)
    for axis in range(3):
        out_ref[axis] = acc_ref[:, 4 + axis, :]


def shards(node_state, node_dest, seg_nodes, seg_conn, pair_seg, pair_slot):
    dom_count = lax.axis_size("dom")
    grp_count = lax.axis_size("grp")
    devices = dom_count * grp_count
    block_count = node_state.shape[0]
    capacity = max(2, 2 * block_count // dom_count)
    width = pair_seg.shape[2]
    seg_blocks = seg_conn.shape[1] // BLK
    rows = devices * width // BLK
    message = pl.pallas_call(
        geometry_kernel,
        out_shape=jax.ShapeDtypeStruct((seg_blocks + 1, 8, BLK), F32),
        in_specs=[VMEM] * 4,
        out_specs=VMEM,
    )(seg_nodes, seg_conn, pair_seg, pair_slot)
    gathered = lax.all_gather(message, ("grp", "dom"), axis=0, tiled=False)
    gathered = gathered.reshape(devices, seg_blocks + 1, 8, BLK)
    force = pl.pallas_call(
        functools.partial(force_kernel, dom_count, capacity, width),
        out_shape=jax.ShapeDtypeStruct((3, block_count, BLK), F32),
        in_specs=[VMEM] * 3,
        out_specs=VMEM,
        scratch_shapes=[
            pltpu.VMEM((2 * rows + 8, BLK), jnp.int32),
            pltpu.SMEM((2 * rows + 8, BLK), jnp.int32),
            pltpu.VMEM((block_count, 8, BLK), F32),
            pltpu.SemaphoreType.DMA,
        ],
    )(gathered, jnp.transpose(node_state, (1, 0, 2)), node_dest.reshape(1, block_count))
    return jnp.transpose(force, (1, 0, 2))


def solution(mesh):
    in_specs = (
        P(("grp", "dom"), None, None),
        P(("grp", "dom")),
        P(None, ("grp", "dom")),
        P(None, ("grp", "dom")),
        P(("grp", "dom"), None, None),
        P(("grp", "dom"), None, None),
    )
    out_specs = P(("grp", "dom"), None, None)
    return jax.shard_map(shards, mesh=mesh, in_specs=in_specs, out_specs=out_specs, check_vma=False)
```

```python
import functools
import math

import jax
import jax.numpy as jnp
from jax import lax
from jax.experimental import pallas as pl
from jax.experimental.pallas import tpu as pltpu
from jax.sharding import PartitionSpec as P

BLK = 128
time_step = 0.5
stiffness = 0.5
radius_sq = 0.5
ALPHA = -math.log2(math.e) / radius_sq
F32 = jnp.float32
BF16 = jnp.bfloat16
VMEM = pl.BlockSpec(memory_space=pltpu.VMEM)
UNROLL = 4


def iota(shape, axis):
    return lax.broadcasted_iota(jnp.int32, shape, axis)


def write_geometry(seg_nodes, seg_conn, store):
    blocks = seg_conn.shape[1] // BLK
    tiles = seg_nodes.shape[1] // BLK
    corners = []
    for corner in range(3):
        index = jnp.concatenate(
            [seg_conn[corner : corner + 1, b * BLK : (b + 1) * BLK] for b in range(blocks)], axis=0
        )
        tile_id = index // BLK
        lane = index % BLK
        rows = []
        for row in range(6):
            value = None
            for t in range(tiles):
                table = jnp.broadcast_to(
                    seg_nodes[row : row + 1, t * BLK : (t + 1) * BLK], (blocks, BLK)
                )
                picked = jnp.take_along_axis(table, lane, axis=1)
                value = picked if value is None else jnp.where(tile_id == t, picked, value)
            rows.append(value)
        corners.append(rows)
    a, b, c = corners
    one = [b[i] - a[i] for i in range(3)]
    two = [c[i] - a[i] for i in range(3)]
    normal = [
        0.5 * (one[1] * two[2] - one[2] * two[1]),
        0.5 * (one[2] * two[0] - one[0] * two[2]),
        0.5 * (one[0] * two[1] - one[1] * two[0]),
    ]
    mean = [(a[i] + b[i] + c[i]) / 3.0 for i in range(6)]
    norm = mean[0] * mean[0] + mean[1] * mean[1] + mean[2] * mean[2]
    shift = sum(normal[i] * (mean[i] + time_step * mean[3 + i]) for i in range(3))
    for i in range(3):
        store(i, (-2.0 * ALPHA) * mean[i])
        store(4 + i, -stiffness * normal[i])
    store(3, ALPHA * norm)
    store(7, stiffness * shift)


def repeat(count, body):
    if count <= 8:
        for i in range(count):
            body(i)
    else:
        lax.fori_loop(0, count, lambda i, carry: (body(i), carry)[1], 0)


def gather_kernel(
    grp_count, dom_count, nodes_ref, conn_ref, seg_ref, slot_ref, out_ref, z_send, g_send, c_send, recv
):
    blocks = conn_ref.shape[1] // BLK
    groups = seg_ref.shape[1]
    grp = lax.axis_index("grp")
    dom = lax.axis_index("dom")
    core = dom % 2
    level = dom // 2
    levels = dom_count // 2
    me = grp * dom_count + dom

    def peer_level(k):
        return (level + 1 + k) % levels * 2 + core

    def peer_grp(k):
        return (grp + 1 + k) % grp_count

    other = level * 2 + 1 - core
    barrier = pltpu.get_barrier_semaphore()
    mesh_id = pl.DeviceIdType.MESH
    repeat(
        levels - 1,
        lambda k: pl.semaphore_signal(
            barrier, inc=1, device_id=(grp, peer_level(k)), device_id_type=mesh_id
        ),
    )
    for k in range(grp_count - 1):
        pl.semaphore_signal(barrier, inc=1, device_id=(peer_grp(k), dom), device_id_type=mesh_id)
    pl.semaphore_signal(barrier, inc=1, device_id=(grp, other), device_id_type=mesh_id)

    def store(row, value):
        out_ref[me, 0:blocks, row, :] = value

    write_geometry(nodes_ref[...], conn_ref[...], store)
    for row, ref in ((0, seg_ref), (1, slot_ref)):
        flat = jnp.concatenate([ref[0, r : r + 1, :] for r in range(groups)], axis=1)
        out_ref[me, blocks, row : row + 1, :] = flat.astype(F32)
    out_ref[me, blocks, 2:8, :] = jnp.zeros((6, BLK), F32)
    pl.semaphore_wait(barrier, levels - 1 + grp_count - 1 + 1)

    def copy(source, send, to):
        return pltpu.make_async_remote_copy(
            src_ref=out_ref.at[source],
            dst_ref=out_ref.at[source],
            send_sem=send,
            recv_sem=recv.at[source],
            device_id=to,
            device_id_type=mesh_id,
        )

    def z_copy(k):
        return copy(me, z_send.at[k], (grp, peer_level(k)))

    def g_copy(source, slot, k):
        return copy(source, g_send.at[slot * (grp_count - 1) + k], (peer_grp(k), dom))

    def c_copy(source):
        return copy(source, c_send.at[source], (grp, other))

    def spread(source, slot):
        for k in range(grp_count - 1):
            g_copy(source, slot, k).start()
        c_copy(source).start()

    def arrive(source):
        c_copy(source).wait_recv()

    repeat(levels - 1, lambda k: z_copy(k).start())
    spread(me, levels - 1)

    def pass_z(k):
        source = grp * dom_count + peer_level(k)
        arrive(source)
        spread(source, k)

    def pass_g(k):
        for j in range(grp_count - 1):
            source = peer_grp(j) * dom_count + peer_level(k)
            arrive(source)
            c_copy(source).start()

    pass_g(levels - 1)
    repeat(levels - 1, pass_z)
    repeat(levels - 1, pass_g)

    def settle(k):
        level_id = (level + 1 + k) % levels * 2
        for j in range(grp_count):
            row = (grp + j) % grp_count * dom_count
            arrive(row + level_id + 1 - core)
            c_copy(row + level_id + core).wait_send()
        for j in range(grp_count - 1):
            g_copy(me, k, j).wait_send()

    repeat(levels, settle)
    repeat(levels - 1, lambda k: z_copy(k).wait_send())


def pack_lanes(value, rows):
    return jnp.concatenate(
        [value[i * rows : (i + 1) * rows] for i in range(value.shape[0] // rows)], axis=1
    )


def pair_list(seg, slot, dest, my_dom, dom_count, seg_blocks, capacity, width):
    rows = seg.shape[0]
    nb = dest.shape[1]
    spread = jnp.broadcast_to(dest.astype(F32), (nb, nb))
    column = spread.T
    lower = iota((nb, nb), 1) < iota((nb, nb), 0)
    rank = jnp.sum(jnp.where((spread == column) & lower, 1.0, 0.0), axis=1, keepdims=True)
    own_key = column * float(capacity) + rank

    source = (iota((rows, BLK), 1) // width) * rows + iota((rows, BLK), 0)
    mine = slot // capacity == my_dom
    key = ((source % dom_count) * capacity + slot % capacity).astype(F32)
    block = source * seg_blocks + seg
    mask = jnp.where(mine, 1.0, 0.0)
    strict = jnp.where(iota((BLK, BLK), 0) < iota((BLK, BLK), 1), 1.0, 0.0)
    before = jnp.dot(mask.astype(BF16), strict.astype(BF16), preferred_element_type=F32)
    above = jnp.where(iota((rows, rows), 1) < iota((rows, rows), 0), 1.0, 0.0)
    ahead = jnp.sum(
        jnp.dot(above.astype(BF16), mask.astype(BF16), preferred_element_type=F32),
        axis=1,
        keepdims=True,
    )
    position = (before + ahead).astype(jnp.int32)
    count = jnp.sum(mask)
    high = jnp.where(mine, position // BLK, -1)
    low = position % BLK
    node_iota = iota((nb, BLK), 0).astype(F32)
    total = jnp.zeros((3 * rows, BLK), F32)
    for row in range(rows):
        cut = slice(row, row + 1)
        node = jnp.sum(jnp.where(own_key == key[cut], node_iota, 0.0), axis=0, keepdims=True)
        hot = jnp.where(iota((BLK, BLK), 0) == low[cut], 1.0, 0.0).astype(BF16)
        here = iota((rows, BLK), 0) == high[cut]
        codes = [node, (block[cut] % 256).astype(F32), (block[cut] // 256).astype(F32)]
        lhs = jnp.concatenate([jnp.where(here, code, 0.0) for code in codes], axis=0)
        total = total + lax.dot_general(
            lhs.astype(BF16), hot, (((1,), (1,)), ((), ())), preferred_element_type=F32
        )
    total = total.astype(jnp.int32)
    return total[0:rows], total[rows : 2 * rows] + 256 * total[2 * rows : 3 * rows], count


def split3(value):
    hi = value.astype(BF16).astype(F32)
    rest = value - hi
    mid = rest.astype(BF16).astype(F32)
    return hi, mid, rest - mid


def node_side(node):
    place = node[0:3]
    ahead = place + time_step * node[3:6]
    ones = jnp.ones((1, BLK), F32)
    zeros = jnp.zeros((4, BLK), F32)
    square = split3(ALPHA * jnp.sum(place * place, axis=0, keepdims=True))
    pad = jnp.zeros((13, BLK), F32)
    eh, em, el = split3(jnp.concatenate([place, ones, zeros], axis=0))
    ch, cm, cl = split3(jnp.concatenate([zeros, ahead, ones], axis=0))
    left = jnp.concatenate([eh, em, el, eh, em, eh, *square, pad], axis=0)
    right = jnp.concatenate([ch, cm, cl, ch, cm, ch, jnp.zeros((16, BLK), F32)], axis=0)
    return jnp.concatenate([left.astype(BF16), right.astype(BF16)], axis=1)


def pair_force(geo, node):
    hi, mid, lo = split3(geo)
    ones = jnp.ones((16, BLK), F32)
    left = jnp.concatenate([hi, hi, hi, mid, mid, lo, ones], axis=0).astype(BF16)
    both = lax.dot_general(
        left, node_side(node), (((0,), (0,)), ((), ())), preferred_element_type=F32
    )
    pressure = jnp.exp2(both[:, 0:BLK]) * jnp.maximum(both[:, BLK:], 0.0)
    top = pressure.astype(BF16)
    bottom = (pressure - top.astype(F32)).astype(BF16)
    weights = jnp.concatenate([hi, mid], axis=0).astype(BF16)
    result = jnp.dot(
        jnp.concatenate([weights, weights], axis=1),
        jnp.concatenate([top, bottom], axis=0),
        preferred_element_type=F32,
    )
    return result[0:8] + result[8:16]


def force_kernel(
    dom_count, capacity, width, geo_ref, node_ref, dest_ref, out_ref, list_vmem, list_smem, acc_ref, sem
):
    my_dom = lax.axis_index("dom")
    my_row = lax.axis_index("grp")
    devices, planes = geo_ref.shape[0], geo_ref.shape[1]
    seg_blocks = planes - 1
    rows = devices * width // BLK
    tables = []
    for row in range(2):
        full = geo_ref[:, seg_blocks, row, :]
        value = None
        for r in range(BLK // width):
            piece = full[:, r * width : (r + 1) * width]
            value = piece if value is None else jnp.where(my_row == r, piece, value)
        tables.append(pack_lanes(value, rows).astype(jnp.int32))
    nodes, blocks, count = pair_list(
        tables[0], tables[1], dest_ref[...], my_dom, dom_count, seg_blocks, capacity, width
    )
    list_vmem[0:rows] = nodes
    list_vmem[rows : 2 * rows] = blocks
    list_vmem[2 * rows : 2 * rows + 1] = jnp.full((1, BLK), count, F32).astype(jnp.int32)
    copy = pltpu.make_async_copy(list_vmem, list_smem, sem)
    copy.start()
    acc_ref[...] = jnp.zeros_like(acc_ref)
    copy.wait()
    pairs = list_smem[2 * rows, 0]

    def body(step, carry):
        results = []
        for u in range(UNROLL):
            p = jnp.minimum(step * UNROLL + u, rows * BLK - 1)
            node_id = list_smem[p // BLK, p % BLK]
            block_id = list_smem[rows + p // BLK, p % BLK]
            geo = geo_ref[block_id // seg_blocks, block_id % seg_blocks]
            results.append((p, node_id, pair_force(geo, node_ref[:, node_id, :])))
        for u in range(UNROLL):
            p, node_id, force = results[u]
            scale = jnp.where(step * UNROLL + u < pairs, -1.0 / stiffness, 0.0)
            acc_ref[node_id] = acc_ref[node_id] + scale * force
        return carry

    lax.fori_loop(0, (pairs + UNROLL - 1) // UNROLL, body, 0)
    for axis in range(3):
        out_ref[axis] = acc_ref[:, 4 + axis, :]


def shards(node_state, node_dest, seg_nodes, seg_conn, pair_seg, pair_slot):
    dom_count = lax.axis_size("dom")
    grp_count = lax.axis_size("grp")
    devices = dom_count * grp_count
    block_count = node_state.shape[0]
    capacity = max(2, 2 * block_count // dom_count)
    width = pair_seg.shape[2]
    seg_blocks = seg_conn.shape[1] // BLK
    rows = devices * width // BLK
    gathered = pl.pallas_call(
        functools.partial(gather_kernel, grp_count, dom_count),
        out_shape=jax.ShapeDtypeStruct((devices, seg_blocks + 1, 8, BLK), F32),
        in_specs=[VMEM] * 4,
        out_specs=VMEM,
        scratch_shapes=[
            pltpu.SemaphoreType.DMA((dom_count // 2,)),
            pltpu.SemaphoreType.DMA((dom_count // 2 * (grp_count - 1),)),
            pltpu.SemaphoreType.DMA((devices,)),
            pltpu.SemaphoreType.DMA((devices,)),
        ],
        compiler_params=pltpu.CompilerParams(collective_id=0, has_side_effects=True),
    )(seg_nodes, seg_conn, pair_seg, pair_slot)
    force = pl.pallas_call(
        functools.partial(force_kernel, dom_count, capacity, width),
        out_shape=jax.ShapeDtypeStruct((3, block_count, BLK), F32),
        in_specs=[VMEM] * 3,
        out_specs=VMEM,
        scratch_shapes=[
            pltpu.VMEM((2 * rows + 8, BLK), jnp.int32),
            pltpu.SMEM((2 * rows + 8, BLK), jnp.int32),
            pltpu.VMEM((block_count, 8, BLK), F32),
            pltpu.SemaphoreType.DMA,
        ],
    )(gathered, jnp.transpose(node_state, (1, 0, 2)), node_dest.reshape(1, block_count))
    return jnp.transpose(force, (1, 0, 2))


def solution(mesh):
    in_specs = (
        P(("grp", "dom"), None, None),
        P(("grp", "dom")),
        P(None, ("grp", "dom")),
        P(None, ("grp", "dom")),
        P(("grp", "dom"), None, None),
        P(("grp", "dom"), None, None),
    )
    out_specs = P(("grp", "dom"), None, None)
    return jax.shard_map(shards, mesh=mesh, in_specs=in_specs, out_specs=out_specs, check_vma=False)
```

```python
import functools
import math

import jax
import jax.numpy as jnp
from jax import lax
from jax.experimental import pallas as pl
from jax.experimental.pallas import tpu as pltpu
from jax.sharding import PartitionSpec as P

BLK = 128
time_step = 0.5
stiffness = 0.5
radius_sq = 0.5
ALPHA = -math.log2(math.e) / radius_sq
F32 = jnp.float32
BF16 = jnp.bfloat16
VMEM = pl.BlockSpec(memory_space=pltpu.VMEM)
UNROLL = 8


def iota(shape, axis):
    return lax.broadcasted_iota(jnp.int32, shape, axis)


def write_geometry(seg_nodes, seg_conn, store):
    blocks = seg_conn.shape[1] // BLK
    tiles = seg_nodes.shape[1] // BLK
    corners = []
    for corner in range(3):
        index = jnp.concatenate(
            [seg_conn[corner : corner + 1, b * BLK : (b + 1) * BLK] for b in range(blocks)], axis=0
        )
        tile_id = index // BLK
        lane = index % BLK
        rows = []
        for row in range(6):
            value = None
            for t in range(tiles):
                table = jnp.broadcast_to(
                    seg_nodes[row : row + 1, t * BLK : (t + 1) * BLK], (blocks, BLK)
                )
                picked = jnp.take_along_axis(table, lane, axis=1)
                value = picked if value is None else jnp.where(tile_id == t, picked, value)
            rows.append(value)
        corners.append(rows)
    a, b, c = corners
    one = [b[i] - a[i] for i in range(3)]
    two = [c[i] - a[i] for i in range(3)]
    normal = [
        0.5 * (one[1] * two[2] - one[2] * two[1]),
        0.5 * (one[2] * two[0] - one[0] * two[2]),
        0.5 * (one[0] * two[1] - one[1] * two[0]),
    ]
    mean = [(a[i] + b[i] + c[i]) / 3.0 for i in range(6)]
    norm = mean[0] * mean[0] + mean[1] * mean[1] + mean[2] * mean[2]
    shift = sum(normal[i] * (mean[i] + time_step * mean[3 + i]) for i in range(3))
    for i in range(3):
        store(i, (-2.0 * ALPHA) * mean[i])
        store(3 + i, -stiffness * normal[i])
    store(6, ALPHA * norm)
    store(7, stiffness * shift)


def repeat(count, body):
    if count <= 8:
        for i in range(count):
            body(i)
    else:
        lax.fori_loop(0, count, lambda i, carry: (body(i), carry)[1], 0)


def gather_kernel(
    grp_count,
    dom_count,
    nodes_ref,
    conn_ref,
    seg_ref,
    slot_ref,
    state_ref,
    out_ref,
    left_ref,
    z_send,
    g_send,
    c_send,
    recv,
):
    blocks = conn_ref.shape[1] // BLK
    groups = seg_ref.shape[1]
    grp = lax.axis_index("grp")
    dom = lax.axis_index("dom")
    core = dom % 2
    level = dom // 2
    levels = dom_count // 2
    me = grp * dom_count + dom

    def peer_level(k):
        return (level + 1 + k) % levels * 2 + core

    def peer_grp(k):
        return (grp + 1 + k) % grp_count

    other = level * 2 + 1 - core
    barrier = pltpu.get_barrier_semaphore()
    mesh_id = pl.DeviceIdType.MESH
    repeat(
        levels - 1,
        lambda k: pl.semaphore_signal(
            barrier, inc=1, device_id=(grp, peer_level(k)), device_id_type=mesh_id
        ),
    )
    for k in range(grp_count - 1):
        pl.semaphore_signal(barrier, inc=1, device_id=(peer_grp(k), dom), device_id_type=mesh_id)
    pl.semaphore_signal(barrier, inc=1, device_id=(grp, other), device_id_type=mesh_id)

    def store(row, value):
        out_ref[me, 0:blocks, row, :] = value

    write_geometry(nodes_ref[...], conn_ref[...], store)
    for row, ref in ((0, seg_ref), (1, slot_ref)):
        flat = jnp.concatenate([ref[0, r : r + 1, :] for r in range(groups)], axis=1)
        out_ref[me, blocks, row : row + 1, :] = flat.astype(F32)
    out_ref[me, blocks, 2:8, :] = jnp.zeros((6, BLK), F32)
    pl.semaphore_wait(barrier, levels - 1 + grp_count - 1 + 1)

    def copy(source, send, to):
        return pltpu.make_async_remote_copy(
            src_ref=out_ref.at[source],
            dst_ref=out_ref.at[source],
            send_sem=send,
            recv_sem=recv.at[source],
            device_id=to,
            device_id_type=mesh_id,
        )

    def z_copy(k):
        return copy(me, z_send.at[k], (grp, peer_level(k)))

    def g_copy(source, slot, k):
        return copy(source, g_send.at[slot * (grp_count - 1) + k], (peer_grp(k), dom))

    def c_copy(source):
        return copy(source, c_send.at[source], (grp, other))

    def spread(source, slot):
        for k in range(grp_count - 1):
            g_copy(source, slot, k).start()
        c_copy(source).start()

    def arrive(source):
        c_copy(source).wait_recv()

    quarter = state_ref.shape[1] // 4

    def prepare(part):
        def step(i, carry):
            for u in range(4):
                block = part * quarter + i * 4 + u
                left_ref[block] = node_side(state_ref[:, block, :])
            return carry

        lax.fori_loop(0, quarter // 4, step, 0)

    repeat(levels - 1, lambda k: z_copy(k).start())
    spread(me, levels - 1)
    prepare(0)

    def pass_z(k):
        source = grp * dom_count + peer_level(k)
        arrive(source)
        spread(source, k)

    def pass_g(k):
        for j in range(grp_count - 1):
            source = peer_grp(j) * dom_count + peer_level(k)
            arrive(source)
            c_copy(source).start()

    pass_g(levels - 1)
    prepare(1)
    repeat(levels - 1, pass_z)
    prepare(2)
    repeat(levels - 1, pass_g)
    prepare(3)

    def settle(k):
        level_id = (level + 1 + k) % levels * 2
        for j in range(grp_count):
            row = (grp + j) % grp_count * dom_count
            arrive(row + level_id + 1 - core)
            c_copy(row + level_id + core).wait_send()
        for j in range(grp_count - 1):
            g_copy(me, k, j).wait_send()

    repeat(levels, settle)
    repeat(levels - 1, lambda k: z_copy(k).wait_send())


def pack_lanes(value, rows):
    return jnp.concatenate(
        [value[i * rows : (i + 1) * rows] for i in range(value.shape[0] // rows)], axis=1
    )


def pair_list(seg, slot, dest, my_dom, dom_count, seg_blocks, capacity, width):
    rows = seg.shape[0]
    nb = dest.shape[1]
    spread = jnp.broadcast_to(dest.astype(F32), (nb, nb))
    column = spread.T
    lower = iota((nb, nb), 1) < iota((nb, nb), 0)
    rank = jnp.sum(jnp.where((spread == column) & lower, 1.0, 0.0), axis=1, keepdims=True)
    own_key = column * float(capacity) + rank

    source = (iota((rows, BLK), 1) // width) * rows + iota((rows, BLK), 0)
    mine = slot // capacity == my_dom
    key = ((source % dom_count) * capacity + slot % capacity).astype(F32)
    block = source * seg_blocks + seg
    mask = jnp.where(mine, 1.0, 0.0)
    strict = jnp.where(iota((BLK, BLK), 0) < iota((BLK, BLK), 1), 1.0, 0.0)
    before = jnp.dot(mask.astype(BF16), strict.astype(BF16), preferred_element_type=F32)
    above = jnp.where(iota((rows, rows), 1) < iota((rows, rows), 0), 1.0, 0.0)
    ahead = jnp.sum(
        jnp.dot(above.astype(BF16), mask.astype(BF16), preferred_element_type=F32),
        axis=1,
        keepdims=True,
    )
    position = (before + ahead).astype(jnp.int32)
    count = jnp.sum(mask)
    high = jnp.where(mine, position // BLK, -1)
    low = position % BLK
    node_iota = iota((nb, BLK), 0).astype(F32)
    total = jnp.zeros((3 * rows, BLK), F32)
    for row in range(rows):
        cut = slice(row, row + 1)
        node = jnp.sum(jnp.where(own_key == key[cut], node_iota, 0.0), axis=0, keepdims=True)
        hot = jnp.where(iota((BLK, BLK), 0) == low[cut], 1.0, 0.0).astype(BF16)
        here = iota((rows, BLK), 0) == high[cut]
        codes = [node, (block[cut] % 256).astype(F32), (block[cut] // 256).astype(F32)]
        lhs = jnp.concatenate([jnp.where(here, code, 0.0) for code in codes], axis=0)
        total = total + lax.dot_general(
            lhs.astype(BF16), hot, (((1,), (1,)), ((), ())), preferred_element_type=F32
        )
    total = total.astype(jnp.int32)
    return total[0:rows], total[rows : 2 * rows] + 256 * total[2 * rows : 3 * rows], count


def split3(value):
    hi = value.astype(BF16).astype(F32)
    rest = value - hi
    mid = rest.astype(BF16).astype(F32)
    return hi, mid, rest - mid


def node_side(node):
    row = iota((8, BLK), 0)
    full = jnp.concatenate([node, jnp.ones((2, BLK), F32)], axis=0)
    ahead = pltpu.roll(full, 3, 0) + time_step * full
    base = jnp.where((row >= 3) & (row < 6), ahead, full)
    place = jnp.where(row < 3, full, 0.0)
    square = split3(ALPHA * jnp.sum(place * place, axis=0, keepdims=True))
    tail = jnp.where(row == 0, square[0], jnp.where(row == 1, square[1], square[2]))
    tail = jnp.where(row < 3, tail, 0.0)
    hi, mid, lo = split3(base)
    rows = jnp.concatenate([hi, mid, lo, hi, mid, hi, tail, jnp.zeros((8, BLK), F32)], axis=0)
    return rows.T.astype(BF16)


def pair_force(geo, node):
    row = iota((8, BLK), 0)
    hi, mid, lo = split3(geo)
    is_e = (row < 3) | (row == 6)
    pieces = [hi, hi, hi, mid, mid, lo]
    left = {id(p): jnp.where(is_e, p, 0.0) for p in (hi, mid, lo)}
    right = {id(p): jnp.where(is_e, 0.0, p) for p in (hi, mid, lo)}
    ones = [jnp.ones((8, BLK), F32)] * 2
    zeros = [jnp.zeros((8, BLK), F32)] * 2
    operand = jnp.concatenate(
        [
            jnp.concatenate([left[id(p)] for p in pieces] + ones, axis=0).astype(BF16),
            jnp.concatenate([right[id(p)] for p in pieces] + zeros, axis=0).astype(BF16),
        ],
        axis=1,
    )
    both = jnp.dot(node, operand, preferred_element_type=F32)
    pressure = jnp.exp2(both[:, 0:BLK]) * jnp.maximum(both[:, BLK:], 0.0)
    top = pressure.astype(BF16)
    bottom = (pressure - top.astype(F32)).astype(BF16)
    weights = jnp.concatenate([hi, mid], axis=0).astype(BF16)
    result = lax.dot_general(
        jnp.concatenate([weights, weights], axis=1),
        jnp.concatenate([top, bottom], axis=1),
        (((1,), (1,)), ((), ())),
        preferred_element_type=F32,
    )
    return result[0:8] + result[8:16]


def force_kernel(
    dom_count, capacity, width, geo_ref, node_ref, dest_ref, out_ref, list_vmem, list_smem, acc_ref, sem
):
    my_dom = lax.axis_index("dom")
    my_row = lax.axis_index("grp")
    devices, planes = geo_ref.shape[0], geo_ref.shape[1]
    seg_blocks = planes - 1
    rows = devices * width // BLK
    tables = []
    for row in range(2):
        full = geo_ref[:, seg_blocks, row, :]
        value = None
        for r in range(BLK // width):
            piece = full[:, r * width : (r + 1) * width]
            value = piece if value is None else jnp.where(my_row == r, piece, value)
        tables.append(pack_lanes(value, rows).astype(jnp.int32))
    nodes, blocks, count = pair_list(
        tables[0], tables[1], dest_ref[...], my_dom, dom_count, seg_blocks, capacity, width
    )
    list_vmem[0:rows] = nodes
    list_vmem[rows : 2 * rows] = blocks
    list_vmem[2 * rows : 2 * rows + 1] = jnp.full((1, BLK), count, F32).astype(jnp.int32)
    copy = pltpu.make_async_copy(list_vmem, list_smem, sem)
    copy.start()
    acc_ref[...] = jnp.zeros_like(acc_ref)
    copy.wait()
    pairs = list_smem[2 * rows, 0]

    def body(step, carry):
        results = []
        for u in range(UNROLL):
            p = jnp.minimum(step * UNROLL + u, rows * BLK - 1)
            node_id = list_smem[p // BLK, p % BLK]
            block_id = list_smem[rows + p // BLK, p % BLK]
            geo = geo_ref[block_id // seg_blocks, block_id % seg_blocks]
            results.append((p, node_id, pair_force(geo, node_ref[node_id])))
        for u in range(UNROLL):
            p, node_id, force = results[u]
            scale = jnp.where(step * UNROLL + u < pairs, -1.0 / stiffness, 0.0)
            acc_ref[node_id] = acc_ref[node_id] + scale * force
        return carry

    lax.fori_loop(0, (pairs + UNROLL - 1) // UNROLL, body, 0)
    for axis in range(3):
        out_ref[axis] = acc_ref[:, 3 + axis, :]


def shards(node_state, node_dest, seg_nodes, seg_conn, pair_seg, pair_slot):
    dom_count = lax.axis_size("dom")
    grp_count = lax.axis_size("grp")
    devices = dom_count * grp_count
    block_count = node_state.shape[0]
    capacity = max(2, 2 * block_count // dom_count)
    width = pair_seg.shape[2]
    seg_blocks = seg_conn.shape[1] // BLK
    rows = devices * width // BLK
    gathered, left = pl.pallas_call(
        functools.partial(gather_kernel, grp_count, dom_count),
        out_shape=(
            jax.ShapeDtypeStruct((devices, seg_blocks + 1, 8, BLK), F32),
            jax.ShapeDtypeStruct((block_count, BLK, 64), BF16),
        ),
        in_specs=[VMEM] * 5,
        out_specs=(VMEM, VMEM),
        scratch_shapes=[
            pltpu.SemaphoreType.DMA((dom_count // 2,)),
            pltpu.SemaphoreType.DMA((dom_count // 2 * (grp_count - 1),)),
            pltpu.SemaphoreType.DMA((devices,)),
            pltpu.SemaphoreType.DMA((devices,)),
        ],
        compiler_params=pltpu.CompilerParams(collective_id=0, has_side_effects=True),
    )(seg_nodes, seg_conn, pair_seg, pair_slot, jnp.transpose(node_state, (1, 0, 2)))
    force = pl.pallas_call(
        functools.partial(force_kernel, dom_count, capacity, width),
        out_shape=jax.ShapeDtypeStruct((3, block_count, BLK), F32),
        in_specs=[VMEM] * 3,
        out_specs=VMEM,
        scratch_shapes=[
            pltpu.VMEM((2 * rows + 8, BLK), jnp.int32),
            pltpu.SMEM((2 * rows + 8, BLK), jnp.int32),
            pltpu.VMEM((block_count, 8, BLK), F32),
            pltpu.SemaphoreType.DMA,
        ],
    )(gathered, left, node_dest.reshape(1, block_count))
    return jnp.transpose(force, (1, 0, 2))


def solution(mesh):
    in_specs = (
        P(("grp", "dom"), None, None),
        P(("grp", "dom")),
        P(None, ("grp", "dom")),
        P(None, ("grp", "dom")),
        P(("grp", "dom"), None, None),
        P(("grp", "dom"), None, None),
    )
    out_specs = P(("grp", "dom"), None, None)
    return jax.shard_map(shards, mesh=mesh, in_specs=in_specs, out_specs=out_specs, check_vma=False)
```

```python
import functools
import math

import jax
import jax.numpy as jnp
from jax import lax
from jax.experimental import pallas as pl
from jax.experimental.pallas import tpu as pltpu
from jax.sharding import PartitionSpec as P

BLK = 128
time_step = 0.5
stiffness = 0.5
radius_sq = 0.5
ALPHA = -math.log2(math.e) / radius_sq
F32 = jnp.float32
BF16 = jnp.bfloat16
VMEM = pl.BlockSpec(memory_space=pltpu.VMEM)
UNROLL = 8


def iota(shape, axis):
    return lax.broadcasted_iota(jnp.int32, shape, axis)


def write_geometry(seg_nodes, seg_conn, store):
    blocks = seg_conn.shape[1] // BLK
    tiles = seg_nodes.shape[1] // BLK
    corners = []
    for corner in range(3):
        index = jnp.concatenate(
            [seg_conn[corner : corner + 1, b * BLK : (b + 1) * BLK] for b in range(blocks)], axis=0
        )
        tile_id = index // BLK
        lane = index % BLK
        rows = []
        for row in range(6):
            value = None
            for t in range(tiles):
                table = jnp.broadcast_to(
                    seg_nodes[row : row + 1, t * BLK : (t + 1) * BLK], (blocks, BLK)
                )
                picked = jnp.take_along_axis(table, lane, axis=1)
                value = picked if value is None else jnp.where(tile_id == t, picked, value)
            rows.append(value)
        corners.append(rows)
    a, b, c = corners
    one = [b[i] - a[i] for i in range(3)]
    two = [c[i] - a[i] for i in range(3)]
    normal = [
        0.5 * (one[1] * two[2] - one[2] * two[1]),
        0.5 * (one[2] * two[0] - one[0] * two[2]),
        0.5 * (one[0] * two[1] - one[1] * two[0]),
    ]
    mean = [(a[i] + b[i] + c[i]) / 3.0 for i in range(6)]
    norm = mean[0] * mean[0] + mean[1] * mean[1] + mean[2] * mean[2]
    shift = sum(normal[i] * (mean[i] + time_step * mean[3 + i]) for i in range(3))
    for i in range(3):
        store(i, (-2.0 * ALPHA) * mean[i])
        store(3 + i, -stiffness * normal[i])
    store(6, ALPHA * norm)
    store(7, stiffness * shift)


def repeat(count, body):
    if count <= 8:
        for i in range(count):
            body(i)
    else:
        lax.fori_loop(0, count, lambda i, carry: (body(i), carry)[1], 0)


def gather_kernel(
    grp_count,
    dom_count,
    nodes_ref,
    conn_ref,
    seg_ref,
    slot_ref,
    state_ref,
    out_ref,
    left_ref,
    z_send,
    g_send,
    c_send,
    recv,
):
    blocks = conn_ref.shape[1] // BLK
    groups = seg_ref.shape[1]
    grp = lax.axis_index("grp")
    dom = lax.axis_index("dom")
    core = dom % 2
    level = dom // 2
    levels = dom_count // 2
    me = grp * dom_count + dom

    def peer_level(k):
        return (level + 1 + k) % levels * 2 + core

    def peer_grp(k):
        return (grp + 1 + k) % grp_count

    other = level * 2 + 1 - core
    barrier = pltpu.get_barrier_semaphore()
    mesh_id = pl.DeviceIdType.MESH
    repeat(
        levels - 1,
        lambda k: pl.semaphore_signal(
            barrier, inc=1, device_id=(grp, peer_level(k)), device_id_type=mesh_id
        ),
    )
    for k in range(grp_count - 1):
        pl.semaphore_signal(barrier, inc=1, device_id=(peer_grp(k), dom), device_id_type=mesh_id)
    pl.semaphore_signal(barrier, inc=1, device_id=(grp, other), device_id_type=mesh_id)

    def store(row, value):
        out_ref[me, 0:blocks, row, :] = value

    write_geometry(nodes_ref[...], conn_ref[...], store)
    for row, ref in ((0, seg_ref), (1, slot_ref)):
        flat = jnp.concatenate([ref[0, r : r + 1, :] for r in range(groups)], axis=1)
        out_ref[me, blocks, row : row + 1, :] = flat.astype(F32)
    out_ref[me, blocks, 2:8, :] = jnp.zeros((6, BLK), F32)
    pl.semaphore_wait(barrier, levels - 1 + grp_count - 1 + 1)

    def copy(source, send, to):
        return pltpu.make_async_remote_copy(
            src_ref=out_ref.at[source],
            dst_ref=out_ref.at[source],
            send_sem=send,
            recv_sem=recv.at[source],
            device_id=to,
            device_id_type=mesh_id,
        )

    def z_copy(k):
        return copy(me, z_send.at[k], (grp, peer_level(k)))

    def g_copy(source, slot, k):
        return copy(source, g_send.at[slot * (grp_count - 1) + k], (peer_grp(k), dom))

    def c_copy(source):
        return copy(source, c_send.at[source], (grp, other))

    def spread(source, slot):
        for k in range(grp_count - 1):
            g_copy(source, slot, k).start()
        c_copy(source).start()

    def arrive(source):
        c_copy(source).wait_recv()

    quarter = state_ref.shape[1] // 4

    def prepare(part):
        def step(i, carry):
            for u in range(4):
                block = part * quarter + i * 4 + u
                left_ref[block] = node_side(state_ref[:, block, :])
            return carry

        lax.fori_loop(0, quarter // 4, step, 0)

    repeat(levels - 1, lambda k: z_copy(k).start())
    spread(me, levels - 1)
    prepare(0)

    def pass_z(k):
        source = grp * dom_count + peer_level(k)
        arrive(source)
        spread(source, k)

    def pass_g(k):
        for j in range(grp_count - 1):
            source = peer_grp(j) * dom_count + peer_level(k)
            arrive(source)
            c_copy(source).start()

    pass_g(levels - 1)
    prepare(1)
    repeat(levels - 1, pass_z)
    prepare(2)
    repeat(levels - 1, pass_g)
    prepare(3)

    def settle(k):
        level_id = (level + 1 + k) % levels * 2
        for j in range(grp_count):
            row = (grp + j) % grp_count * dom_count
            arrive(row + level_id + 1 - core)
            c_copy(row + level_id + core).wait_send()
        for j in range(grp_count - 1):
            g_copy(me, k, j).wait_send()

    repeat(levels, settle)
    repeat(levels - 1, lambda k: z_copy(k).wait_send())


def pack_lanes(value, rows):
    return jnp.concatenate(
        [value[i * rows : (i + 1) * rows] for i in range(value.shape[0] // rows)], axis=1
    )


def pair_list(seg, slot, dest, my_dom, dom_count, seg_blocks, capacity, width):
    rows = seg.shape[0]
    nb = dest.shape[1]
    spread = jnp.broadcast_to(dest.astype(F32), (nb, nb))
    column = spread.T
    lower = iota((nb, nb), 1) < iota((nb, nb), 0)
    rank = jnp.sum(jnp.where((spread == column) & lower, 1.0, 0.0), axis=1, keepdims=True)
    own_key = column * float(capacity) + rank

    source = (iota((rows, BLK), 1) // width) * rows + iota((rows, BLK), 0)
    mine = slot // capacity == my_dom
    key = ((source % dom_count) * capacity + slot % capacity).astype(F32)
    block = source * seg_blocks + seg
    mask = jnp.where(mine, 1.0, 0.0)
    strict = jnp.where(iota((BLK, BLK), 0) < iota((BLK, BLK), 1), 1.0, 0.0)
    before = jnp.dot(mask.astype(BF16), strict.astype(BF16), preferred_element_type=F32)
    above = jnp.where(iota((rows, rows), 1) < iota((rows, rows), 0), 1.0, 0.0)
    ahead = jnp.sum(
        jnp.dot(above.astype(BF16), mask.astype(BF16), preferred_element_type=F32),
        axis=1,
        keepdims=True,
    )
    position = (before + ahead).astype(jnp.int32)
    count = jnp.sum(mask)
    high = jnp.where(mine, position // BLK, -1)
    low = position % BLK
    node_iota = iota((nb, BLK), 0).astype(F32)
    total = jnp.zeros((3 * rows, BLK), F32)
    for row in range(rows):
        cut = slice(row, row + 1)
        node = jnp.sum(jnp.where(own_key == key[cut], node_iota, 0.0), axis=0, keepdims=True)
        hot = jnp.where(iota((BLK, BLK), 0) == low[cut], 1.0, 0.0).astype(BF16)
        here = iota((rows, BLK), 0) == high[cut]
        codes = [node, (block[cut] % 256).astype(F32), (block[cut] // 256).astype(F32)]
        lhs = jnp.concatenate([jnp.where(here, code, 0.0) for code in codes], axis=0)
        total = total + lax.dot_general(
            lhs.astype(BF16), hot, (((1,), (1,)), ((), ())), preferred_element_type=F32
        )
    total = total.astype(jnp.int32)
    return total[0:rows], total[rows : 2 * rows] + 256 * total[2 * rows : 3 * rows], count


def split3(value):
    hi = value.astype(BF16).astype(F32)
    rest = value - hi
    mid = rest.astype(BF16).astype(F32)
    return hi, mid, rest - mid


def node_side(node):
    row = iota((8, BLK), 0)
    full = jnp.concatenate([node, jnp.ones((2, BLK), F32)], axis=0)
    ahead = pltpu.roll(full, 3, 0) + time_step * full
    base = jnp.where((row >= 3) & (row < 6), ahead, full)
    place = jnp.where(row < 3, full, 0.0)
    square = split3(ALPHA * jnp.sum(place * place, axis=0, keepdims=True))
    tail = jnp.where(row == 0, square[0], jnp.where(row == 1, square[1], square[2]))
    tail = jnp.where(row < 3, tail, 0.0)
    hi, mid, lo = split3(base)
    rows = jnp.concatenate([hi, mid, lo, hi, mid, hi, tail, jnp.zeros((8, BLK), F32)], axis=0)
    return rows.T.astype(BF16)


def pair_force(geo, node):
    row = iota((8, BLK), 0)
    hi, mid, lo = split3(geo)
    is_e = (row < 3) | (row == 6)
    pieces = [hi, hi, hi, mid, mid, lo]
    left = {id(p): jnp.where(is_e, p, 0.0) for p in (hi, mid, lo)}
    right = {id(p): jnp.where(is_e, 0.0, p) for p in (hi, mid, lo)}
    ones = [jnp.ones((8, BLK), F32)] * 2
    zeros = [jnp.zeros((8, BLK), F32)] * 2
    operand = jnp.concatenate(
        [
            jnp.concatenate([left[id(p)] for p in pieces] + ones, axis=0).astype(BF16),
            jnp.concatenate([right[id(p)] for p in pieces] + zeros, axis=0).astype(BF16),
        ],
        axis=1,
    )
    both = jnp.dot(node, operand, preferred_element_type=F32)
    pressure = jnp.exp2(both[:, 0:BLK]) * jnp.maximum(both[:, BLK:], 0.0)
    top = pressure.astype(BF16)
    bottom = (pressure - top.astype(F32)).astype(BF16)
    weights = jnp.concatenate([hi, mid], axis=0).astype(BF16)
    result = lax.dot_general(
        jnp.concatenate([weights, weights], axis=1),
        jnp.concatenate([top, bottom], axis=1),
        (((1,), (1,)), ((), ())),
        preferred_element_type=F32,
    )
    return result[0:8] + result[8:16]


def force_kernel(
    dom_count, capacity, width, geo_ref, node_ref, dest_ref, out_ref, list_vmem, list_smem, acc_ref, sem
):
    my_dom = lax.axis_index("dom")
    my_row = lax.axis_index("grp")
    devices, planes = geo_ref.shape[0], geo_ref.shape[1]
    seg_blocks = planes - 1
    rows = devices * width // BLK
    tables = []
    for row in range(2):
        full = geo_ref[:, seg_blocks, row, :]
        value = None
        for r in range(BLK // width):
            piece = full[:, r * width : (r + 1) * width]
            value = piece if value is None else jnp.where(my_row == r, piece, value)
        tables.append(pack_lanes(value, rows).astype(jnp.int32))
    nodes, blocks, count = pair_list(
        tables[0], tables[1], dest_ref[...], my_dom, dom_count, seg_blocks, capacity, width
    )
    list_vmem[0:rows] = nodes
    list_vmem[rows : 2 * rows] = blocks
    list_vmem[2 * rows : 2 * rows + 1] = jnp.full((1, BLK), count, F32).astype(jnp.int32)
    copy = pltpu.make_async_copy(list_vmem, list_smem, sem)
    copy.start()
    acc_ref[...] = jnp.zeros_like(acc_ref)
    copy.wait()
    pairs = list_smem[2 * rows, 0]

    def body(step, carry):
        results = []
        for u in range(UNROLL):
            p = jnp.minimum(step * UNROLL + u, rows * BLK - 1)
            node_id = list_smem[p // BLK, p % BLK]
            block_id = list_smem[rows + p // BLK, p % BLK]
            geo = geo_ref[block_id // seg_blocks, block_id % seg_blocks]
            results.append((p, node_id, pair_force(geo, node_ref[node_id])))
        for u in range(UNROLL):
            p, node_id, force = results[u]
            scale = jnp.where(step * UNROLL + u < pairs, -1.0 / stiffness, 0.0)
            acc_ref[node_id] = acc_ref[node_id] + scale * force
        return carry

    lax.fori_loop(0, (pairs + UNROLL - 1) // UNROLL, body, 0)
    for axis in range(3):
        out_ref[axis] = acc_ref[:, 3 + axis, :]


def shards(node_state, node_dest, seg_nodes, seg_conn, pair_seg, pair_slot):
    dom_count = lax.axis_size("dom")
    grp_count = lax.axis_size("grp")
    devices = dom_count * grp_count
    block_count = node_state.shape[0]
    capacity = max(2, 2 * block_count // dom_count)
    width = pair_seg.shape[2]
    seg_blocks = seg_conn.shape[1] // BLK
    rows = devices * width // BLK
    vmem_limit = 24 * 2**20
    gathered, left = pl.pallas_call(
        functools.partial(gather_kernel, grp_count, dom_count),
        out_shape=(
            pltpu.VMEM((devices, seg_blocks + 1, 8, BLK), F32),
            pltpu.VMEM((block_count, BLK, 64), BF16),
        ),
        in_specs=[VMEM] * 5,
        out_specs=(VMEM, VMEM),
        scratch_shapes=[
            pltpu.SemaphoreType.DMA((dom_count // 2,)),
            pltpu.SemaphoreType.DMA((dom_count // 2 * (grp_count - 1),)),
            pltpu.SemaphoreType.DMA((devices,)),
            pltpu.SemaphoreType.DMA((devices,)),
        ],
        compiler_params=pltpu.CompilerParams(collective_id=0, has_side_effects=True, vmem_limit_bytes=vmem_limit),
    )(seg_nodes, seg_conn, pair_seg, pair_slot, jnp.transpose(node_state, (1, 0, 2)))
    force = pl.pallas_call(
        functools.partial(force_kernel, dom_count, capacity, width),
        out_shape=jax.ShapeDtypeStruct((3, block_count, BLK), F32),
        in_specs=[VMEM] * 3,
        out_specs=VMEM,
        scratch_shapes=[
            pltpu.VMEM((2 * rows + 8, BLK), jnp.int32),
            pltpu.SMEM((2 * rows + 8, BLK), jnp.int32),
            pltpu.VMEM((block_count, 8, BLK), F32),
            pltpu.SemaphoreType.DMA,
        ],
        compiler_params=pltpu.CompilerParams(vmem_limit_bytes=vmem_limit),
    )(
        pltpu.with_memory_space_constraint(gathered, pltpu.VMEM),
        pltpu.with_memory_space_constraint(left, pltpu.VMEM),
        node_dest.reshape(1, block_count))
    return jnp.transpose(force, (1, 0, 2))


def solution(mesh):
    in_specs = (
        P(("grp", "dom"), None, None),
        P(("grp", "dom")),
        P(None, ("grp", "dom")),
        P(None, ("grp", "dom")),
        P(("grp", "dom"), None, None),
        P(("grp", "dom"), None, None),
    )
    out_specs = P(("grp", "dom"), None, None)
    return jax.shard_map(shards, mesh=mesh, in_specs=in_specs, out_specs=out_specs, check_vma=False)
```

```python
import functools
import math

import jax
import jax.numpy as jnp
from jax import lax
from jax.experimental import pallas as pl
from jax.experimental.pallas import tpu as pltpu
from jax.sharding import PartitionSpec as P

BLK = 128
time_step = 0.5
stiffness = 0.5
radius_sq = 0.5
ALPHA = -math.log2(math.e) / radius_sq
F32 = jnp.float32
BF16 = jnp.bfloat16
VMEM = pl.BlockSpec(memory_space=pltpu.VMEM)
UNROLL = 8


def iota(shape, axis):
    return lax.broadcasted_iota(jnp.int32, shape, axis)


def write_geometry(seg_nodes, seg_conn, store):
    blocks = seg_conn.shape[1] // BLK
    tiles = seg_nodes.shape[1] // BLK
    corners = []
    for corner in range(3):
        index = jnp.concatenate(
            [seg_conn[corner : corner + 1, b * BLK : (b + 1) * BLK] for b in range(blocks)], axis=0
        )
        tile_id = index // BLK
        lane = index % BLK
        rows = []
        for row in range(6):
            value = None
            for t in range(tiles):
                table = jnp.broadcast_to(
                    seg_nodes[row : row + 1, t * BLK : (t + 1) * BLK], (blocks, BLK)
                )
                picked = jnp.take_along_axis(table, lane, axis=1)
                value = picked if value is None else jnp.where(tile_id == t, picked, value)
            rows.append(value)
        corners.append(rows)
    a, b, c = corners
    one = [b[i] - a[i] for i in range(3)]
    two = [c[i] - a[i] for i in range(3)]
    normal = [
        0.5 * (one[1] * two[2] - one[2] * two[1]),
        0.5 * (one[2] * two[0] - one[0] * two[2]),
        0.5 * (one[0] * two[1] - one[1] * two[0]),
    ]
    mean = [(a[i] + b[i] + c[i]) / 3.0 for i in range(6)]
    norm = mean[0] * mean[0] + mean[1] * mean[1] + mean[2] * mean[2]
    shift = sum(normal[i] * (mean[i] + time_step * mean[3 + i]) for i in range(3))
    for i in range(3):
        store(i, (-2.0 * ALPHA) * mean[i])
        store(3 + i, -stiffness * normal[i])
    store(6, ALPHA * norm)
    store(7, stiffness * shift)


def repeat(count, body):
    if count <= 8:
        for i in range(count):
            body(i)
    else:
        lax.fori_loop(0, count, lambda i, carry: (body(i), carry)[1], 0)


def gather_kernel(
    grp_count,
    dom_count,
    nodes_hbm,
    conn_hbm,
    seg_hbm,
    slot_hbm,
    state_hbm,
    dest_hbm,
    out_ref,
    left_ref,
    dest_ref,
    nodes_ref,
    conn_ref,
    seg_ref,
    slot_ref,
    state_ref,
    load_sem,
    z_send,
    g_send,
    c_send,
    recv,
):
    pairs = [
        (nodes_hbm, nodes_ref),
        (conn_hbm, conn_ref),
        (seg_hbm, seg_ref),
        (slot_hbm, slot_ref),
        (state_hbm, state_ref),
        (dest_hbm, dest_ref),
    ]
    loads = [pltpu.make_async_copy(a, b, load_sem.at[i]) for i, (a, b) in enumerate(pairs)]
    for load in loads:
        load.start()
    blocks = conn_ref.shape[1] // BLK
    groups = seg_ref.shape[1]
    grp = lax.axis_index("grp")
    dom = lax.axis_index("dom")
    core = dom % 2
    level = dom // 2
    levels = dom_count // 2
    me = grp * dom_count + dom

    def peer_level(k):
        return (level + 1 + k) % levels * 2 + core

    def peer_grp(k):
        return (grp + 1 + k) % grp_count

    other = level * 2 + 1 - core
    barrier = pltpu.get_barrier_semaphore()
    mesh_id = pl.DeviceIdType.MESH
    repeat(
        levels - 1,
        lambda k: pl.semaphore_signal(
            barrier, inc=1, device_id=(grp, peer_level(k)), device_id_type=mesh_id
        ),
    )
    for k in range(grp_count - 1):
        pl.semaphore_signal(barrier, inc=1, device_id=(peer_grp(k), dom), device_id_type=mesh_id)
    pl.semaphore_signal(barrier, inc=1, device_id=(grp, other), device_id_type=mesh_id)

    def store(row, value):
        out_ref[me, 0:blocks, row, :] = value

    for load in loads[0:4]:
        load.wait()
    write_geometry(nodes_ref[...], conn_ref[...], store)
    for row, ref in ((0, seg_ref), (1, slot_ref)):
        flat = jnp.concatenate([ref[0, r : r + 1, :] for r in range(groups)], axis=1)
        out_ref[me, blocks, row : row + 1, :] = flat.astype(F32)
    out_ref[me, blocks, 2:8, :] = jnp.zeros((6, BLK), F32)
    pl.semaphore_wait(barrier, levels - 1 + grp_count - 1 + 1)

    def copy(source, send, to):
        return pltpu.make_async_remote_copy(
            src_ref=out_ref.at[source],
            dst_ref=out_ref.at[source],
            send_sem=send,
            recv_sem=recv.at[source],
            device_id=to,
            device_id_type=mesh_id,
        )

    def z_copy(k):
        return copy(me, z_send.at[k], (grp, peer_level(k)))

    def g_copy(source, slot, k):
        return copy(source, g_send.at[slot * (grp_count - 1) + k], (peer_grp(k), dom))

    def c_copy(source):
        return copy(source, c_send.at[source], (grp, other))

    def spread(source, slot):
        for k in range(grp_count - 1):
            g_copy(source, slot, k).start()
        c_copy(source).start()

    def arrive(source):
        c_copy(source).wait_recv()

    quarter = state_ref.shape[1] // 4

    def prepare(part):
        def step(i, carry):
            for u in range(4):
                block = part * quarter + i * 4 + u
                left_ref[block] = node_side(state_ref[:, block, :])
            return carry

        lax.fori_loop(0, quarter // 4, step, 0)

    repeat(levels - 1, lambda k: z_copy(k).start())
    spread(me, levels - 1)
    for load in loads[4:]:
        load.wait()
    prepare(0)

    def pass_z(k):
        source = grp * dom_count + peer_level(k)
        arrive(source)
        spread(source, k)

    def pass_g(k):
        for j in range(grp_count - 1):
            source = peer_grp(j) * dom_count + peer_level(k)
            arrive(source)
            c_copy(source).start()

    pass_g(levels - 1)
    prepare(1)
    repeat(levels - 1, pass_z)
    prepare(2)
    repeat(levels - 1, pass_g)
    prepare(3)

    def settle(k):
        level_id = (level + 1 + k) % levels * 2
        for j in range(grp_count):
            row = (grp + j) % grp_count * dom_count
            arrive(row + level_id + 1 - core)
            c_copy(row + level_id + core).wait_send()
        for j in range(grp_count - 1):
            g_copy(me, k, j).wait_send()

    repeat(levels, settle)
    repeat(levels - 1, lambda k: z_copy(k).wait_send())


def pack_lanes(value, rows):
    return jnp.concatenate(
        [value[i * rows : (i + 1) * rows] for i in range(value.shape[0] // rows)], axis=1
    )


def pair_list(seg, slot, dest, my_dom, dom_count, seg_blocks, capacity, width):
    rows = seg.shape[0]
    nb = dest.shape[1]
    spread = jnp.broadcast_to(dest.astype(F32), (nb, nb))
    column = spread.T
    lower = iota((nb, nb), 1) < iota((nb, nb), 0)
    rank = jnp.sum(jnp.where((spread == column) & lower, 1.0, 0.0), axis=1, keepdims=True)
    own_key = column * float(capacity) + rank

    source = (iota((rows, BLK), 1) // width) * rows + iota((rows, BLK), 0)
    mine = slot // capacity == my_dom
    key = ((source % dom_count) * capacity + slot % capacity).astype(F32)
    block = source * seg_blocks + seg
    mask = jnp.where(mine, 1.0, 0.0)
    strict = jnp.where(iota((BLK, BLK), 0) < iota((BLK, BLK), 1), 1.0, 0.0)
    before = jnp.dot(mask.astype(BF16), strict.astype(BF16), preferred_element_type=F32)
    above = jnp.where(iota((rows, rows), 1) < iota((rows, rows), 0), 1.0, 0.0)
    ahead = jnp.sum(
        jnp.dot(above.astype(BF16), mask.astype(BF16), preferred_element_type=F32),
        axis=1,
        keepdims=True,
    )
    position = (before + ahead).astype(jnp.int32)
    count = jnp.sum(mask)
    high = jnp.where(mine, position // BLK, -1)
    low = position % BLK
    node_iota = iota((nb, BLK), 0).astype(F32)
    total = jnp.zeros((3 * rows, BLK), F32)
    for row in range(rows):
        cut = slice(row, row + 1)
        node = jnp.sum(jnp.where(own_key == key[cut], node_iota, 0.0), axis=0, keepdims=True)
        hot = jnp.where(iota((BLK, BLK), 0) == low[cut], 1.0, 0.0).astype(BF16)
        here = iota((rows, BLK), 0) == high[cut]
        codes = [node, (block[cut] % 256).astype(F32), (block[cut] // 256).astype(F32)]
        lhs = jnp.concatenate([jnp.where(here, code, 0.0) for code in codes], axis=0)
        total = total + lax.dot_general(
            lhs.astype(BF16), hot, (((1,), (1,)), ((), ())), preferred_element_type=F32
        )
    total = total.astype(jnp.int32)
    return total[0:rows], total[rows : 2 * rows] + 256 * total[2 * rows : 3 * rows], count


def split3(value):
    hi = value.astype(BF16).astype(F32)
    rest = value - hi
    mid = rest.astype(BF16).astype(F32)
    return hi, mid, rest - mid


def node_side(node):
    row = iota((8, BLK), 0)
    full = jnp.concatenate([node, jnp.ones((2, BLK), F32)], axis=0)
    ahead = pltpu.roll(full, 3, 0) + time_step * full
    base = jnp.where((row >= 3) & (row < 6), ahead, full)
    place = jnp.where(row < 3, full, 0.0)
    square = split3(ALPHA * jnp.sum(place * place, axis=0, keepdims=True))
    tail = jnp.where(row == 0, square[0], jnp.where(row == 1, square[1], square[2]))
    tail = jnp.where(row < 3, tail, 0.0)
    hi, mid, lo = split3(base)
    rows = jnp.concatenate([hi, mid, lo, hi, mid, hi, tail, jnp.zeros((8, BLK), F32)], axis=0)
    return rows.T.astype(BF16)


def pair_force(geo, node):
    row = iota((8, BLK), 0)
    hi, mid, lo = split3(geo)
    is_e = (row < 3) | (row == 6)
    pieces = [hi, hi, hi, mid, mid, lo]
    left = {id(p): jnp.where(is_e, p, 0.0) for p in (hi, mid, lo)}
    right = {id(p): jnp.where(is_e, 0.0, p) for p in (hi, mid, lo)}
    ones = [jnp.ones((8, BLK), F32)] * 2
    zeros = [jnp.zeros((8, BLK), F32)] * 2
    operand = jnp.concatenate(
        [
            jnp.concatenate([left[id(p)] for p in pieces] + ones, axis=0).astype(BF16),
            jnp.concatenate([right[id(p)] for p in pieces] + zeros, axis=0).astype(BF16),
        ],
        axis=1,
    )
    both = jnp.dot(node, operand, preferred_element_type=F32)
    pressure = jnp.exp2(both[:, 0:BLK]) * jnp.maximum(both[:, BLK:], 0.0)
    top = pressure.astype(BF16)
    bottom = (pressure - top.astype(F32)).astype(BF16)
    weights = jnp.concatenate([hi, mid], axis=0).astype(BF16)
    result = lax.dot_general(
        jnp.concatenate([weights, weights], axis=1),
        jnp.concatenate([top, bottom], axis=1),
        (((1,), (1,)), ((), ())),
        preferred_element_type=F32,
    )
    return result[0:8] + result[8:16]


def force_kernel(
    dom_count, capacity, width, geo_ref, node_ref, dest_ref, out_ref, list_vmem, list_smem, acc_ref, sem
):
    my_dom = lax.axis_index("dom")
    my_row = lax.axis_index("grp")
    devices, planes = geo_ref.shape[0], geo_ref.shape[1]
    seg_blocks = planes - 1
    rows = devices * width // BLK
    tables = []
    for row in range(2):
        full = geo_ref[:, seg_blocks, row, :]
        value = None
        for r in range(BLK // width):
            piece = full[:, r * width : (r + 1) * width]
            value = piece if value is None else jnp.where(my_row == r, piece, value)
        tables.append(pack_lanes(value, rows).astype(jnp.int32))
    nodes, blocks, count = pair_list(
        tables[0], tables[1], dest_ref[...], my_dom, dom_count, seg_blocks, capacity, width
    )
    list_vmem[0:rows] = nodes
    list_vmem[rows : 2 * rows] = blocks
    list_vmem[2 * rows : 2 * rows + 1] = jnp.full((1, BLK), count, F32).astype(jnp.int32)
    copy = pltpu.make_async_copy(list_vmem, list_smem, sem)
    copy.start()
    acc_ref[...] = jnp.zeros_like(acc_ref)
    copy.wait()
    pairs = list_smem[2 * rows, 0]

    def body(step, carry):
        results = []
        for u in range(UNROLL):
            p = jnp.minimum(step * UNROLL + u, rows * BLK - 1)
            node_id = list_smem[p // BLK, p % BLK]
            block_id = list_smem[rows + p // BLK, p % BLK]
            geo = geo_ref[block_id // seg_blocks, block_id % seg_blocks]
            results.append((p, node_id, pair_force(geo, node_ref[node_id])))
        for u in range(UNROLL):
            p, node_id, force = results[u]
            scale = jnp.where(step * UNROLL + u < pairs, -1.0 / stiffness, 0.0)
            acc_ref[node_id] = acc_ref[node_id] + scale * force
        return carry

    lax.fori_loop(0, (pairs + UNROLL - 1) // UNROLL, body, 0)
    for axis in range(3):
        out_ref[axis] = acc_ref[:, 3 + axis, :]


def shards(node_state, node_dest, seg_nodes, seg_conn, pair_seg, pair_slot):
    dom_count = lax.axis_size("dom")
    grp_count = lax.axis_size("grp")
    devices = dom_count * grp_count
    block_count = node_state.shape[0]
    capacity = max(2, 2 * block_count // dom_count)
    width = pair_seg.shape[2]
    seg_blocks = seg_conn.shape[1] // BLK
    rows = devices * width // BLK
    vmem_limit = 24 * 2**20
    gathered, left, dest = pl.pallas_call(
        functools.partial(gather_kernel, grp_count, dom_count),
        out_shape=(
            pltpu.VMEM((devices, seg_blocks + 1, 8, BLK), F32),
            pltpu.VMEM((block_count, BLK, 64), BF16),
            pltpu.VMEM((1, block_count), jnp.int32),
        ),
        in_specs=[pl.BlockSpec(memory_space=pltpu.HBM)] * 6,
        out_specs=(VMEM, VMEM, VMEM),
        scratch_shapes=[
            pltpu.VMEM(seg_nodes.shape, F32),
            pltpu.VMEM(seg_conn.shape, jnp.int32),
            pltpu.VMEM(pair_seg.shape, jnp.int32),
            pltpu.VMEM(pair_slot.shape, jnp.int32),
            pltpu.VMEM((6, block_count, BLK), F32),
            pltpu.SemaphoreType.DMA((6,)),
            pltpu.SemaphoreType.DMA((dom_count // 2,)),
            pltpu.SemaphoreType.DMA((dom_count // 2 * (grp_count - 1),)),
            pltpu.SemaphoreType.DMA((devices,)),
            pltpu.SemaphoreType.DMA((devices,)),
        ],
        compiler_params=pltpu.CompilerParams(collective_id=0, has_side_effects=True, vmem_limit_bytes=vmem_limit),
    )(
        *(
            pltpu.with_memory_space_constraint(x, pltpu.HBM)
            for x in (
                seg_nodes,
                seg_conn,
                pair_seg,
                pair_slot,
                jnp.transpose(node_state, (1, 0, 2)),
                node_dest.reshape(1, block_count),
            )
        )
    )
    force = pl.pallas_call(
        functools.partial(force_kernel, dom_count, capacity, width),
        out_shape=jax.ShapeDtypeStruct((3, block_count, BLK), F32),
        in_specs=[VMEM] * 3,
        out_specs=VMEM,
        scratch_shapes=[
            pltpu.VMEM((2 * rows + 8, BLK), jnp.int32),
            pltpu.SMEM((2 * rows + 8, BLK), jnp.int32),
            pltpu.VMEM((block_count, 8, BLK), F32),
            pltpu.SemaphoreType.DMA,
        ],
        compiler_params=pltpu.CompilerParams(vmem_limit_bytes=vmem_limit),
    )(
        pltpu.with_memory_space_constraint(gathered, pltpu.VMEM),
        pltpu.with_memory_space_constraint(left, pltpu.VMEM),
        pltpu.with_memory_space_constraint(dest, pltpu.VMEM),
    )
    return jnp.transpose(force, (1, 0, 2))


def solution(mesh):
    in_specs = (
        P(("grp", "dom"), None, None),
        P(("grp", "dom")),
        P(None, ("grp", "dom")),
        P(None, ("grp", "dom")),
        P(("grp", "dom"), None, None),
        P(("grp", "dom"), None, None),
    )
    out_specs = P(("grp", "dom"), None, None)
    return jax.shard_map(shards, mesh=mesh, in_specs=in_specs, out_specs=out_specs, check_vma=False)
```

```python
import functools
import math

import jax
import jax.numpy as jnp
from jax import lax
from jax.experimental import pallas as pl
from jax.experimental.pallas import tpu as pltpu
from jax.sharding import PartitionSpec as P

BLK = 128
time_step = 0.5
stiffness = 0.5
radius_sq = 0.5
ALPHA = -math.log2(math.e) / radius_sq
F32 = jnp.float32
BF16 = jnp.bfloat16
VMEM = pl.BlockSpec(memory_space=pltpu.VMEM)
UNROLL = 8


def iota(shape, axis):
    return lax.broadcasted_iota(jnp.int32, shape, axis)


def write_geometry(seg_nodes, seg_conn, store):
    blocks = seg_conn.shape[1] // BLK
    tiles = seg_nodes.shape[1] // BLK
    corners = []
    for corner in range(3):
        index = jnp.concatenate(
            [seg_conn[corner : corner + 1, b * BLK : (b + 1) * BLK] for b in range(blocks)], axis=0
        )
        tile_id = index // BLK
        lane = index % BLK
        rows = []
        for row in range(6):
            value = None
            for t in range(tiles):
                table = jnp.broadcast_to(
                    seg_nodes[row : row + 1, t * BLK : (t + 1) * BLK], (blocks, BLK)
                )
                picked = jnp.take_along_axis(table, lane, axis=1)
                value = picked if value is None else jnp.where(tile_id == t, picked, value)
            rows.append(value)
        corners.append(rows)
    a, b, c = corners
    one = [b[i] - a[i] for i in range(3)]
    two = [c[i] - a[i] for i in range(3)]
    normal = [
        0.5 * (one[1] * two[2] - one[2] * two[1]),
        0.5 * (one[2] * two[0] - one[0] * two[2]),
        0.5 * (one[0] * two[1] - one[1] * two[0]),
    ]
    mean = [(a[i] + b[i] + c[i]) / 3.0 for i in range(6)]
    norm = mean[0] * mean[0] + mean[1] * mean[1] + mean[2] * mean[2]
    shift = sum(normal[i] * (mean[i] + time_step * mean[3 + i]) for i in range(3))
    for i in range(3):
        store(i, (-2.0 * ALPHA) * mean[i])
        store(3 + i, -stiffness * normal[i])
    store(6, ALPHA * norm)
    store(7, stiffness * shift)


def repeat(count, body):
    if count <= 8:
        for i in range(count):
            body(i)
    else:
        lax.fori_loop(0, count, lambda i, carry: (body(i), carry)[1], 0)


def gather_kernel(
    grp_count,
    dom_count,
    nodes_hbm,
    conn_hbm,
    seg_hbm,
    slot_hbm,
    state_hbm,
    dest_hbm,
    out_ref,
    left_ref,
    dest_ref,
    nodes_ref,
    conn_ref,
    seg_ref,
    slot_ref,
    state_ref,
    load_sem,
    z_send,
    g_send,
    c_send,
    recv,
):
    pairs = [
        (nodes_hbm, nodes_ref),
        (conn_hbm, conn_ref),
        (seg_hbm, seg_ref),
        (slot_hbm, slot_ref),
        (state_hbm, state_ref),
        (dest_hbm, dest_ref),
    ]
    loads = [pltpu.make_async_copy(a, b, load_sem.at[i]) for i, (a, b) in enumerate(pairs)]
    for load in loads:
        load.start()
    blocks = conn_ref.shape[1] // BLK
    groups = seg_ref.shape[1]
    grp = lax.axis_index("grp")
    dom = lax.axis_index("dom")
    core = dom % 2
    level = dom // 2
    levels = dom_count // 2
    me = grp * dom_count + dom

    def peer_level(k):
        return (level + 1 + k) % levels * 2 + core

    def peer_grp(k):
        return (grp + 1 + k) % grp_count

    other = level * 2 + 1 - core
    barrier = pltpu.get_barrier_semaphore()
    mesh_id = pl.DeviceIdType.MESH
    repeat(
        levels - 1,
        lambda k: pl.semaphore_signal(
            barrier, inc=1, device_id=(grp, peer_level(k)), device_id_type=mesh_id
        ),
    )
    for k in range(grp_count - 1):
        pl.semaphore_signal(barrier, inc=1, device_id=(peer_grp(k), dom), device_id_type=mesh_id)
    pl.semaphore_signal(barrier, inc=1, device_id=(grp, other), device_id_type=mesh_id)

    def store(row, value):
        out_ref[me, 0:blocks, row, :] = value

    for load in loads[0:4]:
        load.wait()
    write_geometry(nodes_ref[...], conn_ref[...], store)
    for row, ref in ((0, seg_ref), (1, slot_ref)):
        flat = jnp.concatenate([ref[0, r : r + 1, :] for r in range(groups)], axis=1)
        out_ref[me, blocks, row : row + 1, :] = flat.astype(F32)
    out_ref[me, blocks, 2:8, :] = jnp.zeros((6, BLK), F32)
    pl.semaphore_wait(barrier, levels - 1 + grp_count - 1 + 1)

    def copy(source, send, to):
        return pltpu.make_async_remote_copy(
            src_ref=out_ref.at[source],
            dst_ref=out_ref.at[source],
            send_sem=send,
            recv_sem=recv.at[source],
            device_id=to,
            device_id_type=mesh_id,
        )

    def z_copy(k):
        return copy(me, z_send.at[k], (grp, peer_level(k)))

    def g_copy(source, slot, k):
        return copy(source, g_send.at[slot * (grp_count - 1) + k], (peer_grp(k), dom))

    def c_copy(source):
        return copy(source, c_send.at[source], (grp, other))

    def spread(source, slot):
        for k in range(grp_count - 1):
            g_copy(source, slot, k).start()
        c_copy(source).start()

    def arrive(source):
        c_copy(source).wait_recv()

    quarter = state_ref.shape[1] // 4

    def prepare(part):
        def step(i, carry):
            for u in range(4):
                block = part * quarter + i * 4 + u
                left_ref[block] = node_side(state_ref[:, block, :])
            return carry

        lax.fori_loop(0, quarter // 4, step, 0)

    repeat(levels - 1, lambda k: z_copy(k).start())
    spread(me, levels - 1)
    for load in loads[4:]:
        load.wait()
    prepare(0)

    def pass_z(k):
        source = grp * dom_count + peer_level(k)
        arrive(source)
        spread(source, k)

    def pass_g(k):
        for j in range(grp_count - 1):
            source = peer_grp(j) * dom_count + peer_level(k)
            arrive(source)
            c_copy(source).start()

    repeat(levels - 1, pass_z)
    pass_g(levels - 1)
    prepare(1)
    prepare(2)
    prepare(3)
    repeat(levels - 1, pass_g)

    def settle(k):
        level_id = (level + 1 + k) % levels * 2
        for j in range(grp_count):
            row = (grp + j) % grp_count * dom_count
            arrive(row + level_id + 1 - core)
            c_copy(row + level_id + core).wait_send()
        for j in range(grp_count - 1):
            g_copy(me, k, j).wait_send()

    repeat(levels, settle)
    repeat(levels - 1, lambda k: z_copy(k).wait_send())


def pack_lanes(value, rows):
    return jnp.concatenate(
        [value[i * rows : (i + 1) * rows] for i in range(value.shape[0] // rows)], axis=1
    )


def pair_list(seg, slot, dest, my_dom, dom_count, seg_blocks, capacity, width):
    rows = seg.shape[0]
    nb = dest.shape[1]
    spread = jnp.broadcast_to(dest.astype(F32), (nb, nb))
    column = spread.T
    lower = iota((nb, nb), 1) < iota((nb, nb), 0)
    rank = jnp.sum(jnp.where((spread == column) & lower, 1.0, 0.0), axis=1, keepdims=True)
    own_key = column * float(capacity) + rank

    source = (iota((rows, BLK), 1) // width) * rows + iota((rows, BLK), 0)
    mine = slot // capacity == my_dom
    key = ((source % dom_count) * capacity + slot % capacity).astype(F32)
    block = source * seg_blocks + seg
    mask = jnp.where(mine, 1.0, 0.0)
    strict = jnp.where(iota((BLK, BLK), 0) < iota((BLK, BLK), 1), 1.0, 0.0)
    before = jnp.dot(mask.astype(BF16), strict.astype(BF16), preferred_element_type=F32)
    above = jnp.where(iota((rows, rows), 1) < iota((rows, rows), 0), 1.0, 0.0)
    ahead = jnp.sum(
        jnp.dot(above.astype(BF16), mask.astype(BF16), preferred_element_type=F32),
        axis=1,
        keepdims=True,
    )
    position = (before + ahead).astype(jnp.int32)
    count = jnp.sum(mask)
    high = jnp.where(mine, position // BLK, -1)
    low = position % BLK
    node_iota = iota((nb, BLK), 0).astype(F32)
    total = jnp.zeros((3 * rows, BLK), F32)
    for row in range(rows):
        cut = slice(row, row + 1)
        node = jnp.sum(jnp.where(own_key == key[cut], node_iota, 0.0), axis=0, keepdims=True)
        hot = jnp.where(iota((BLK, BLK), 0) == low[cut], 1.0, 0.0).astype(BF16)
        here = iota((rows, BLK), 0) == high[cut]
        codes = [node, (block[cut] % 256).astype(F32), (block[cut] // 256).astype(F32)]
        lhs = jnp.concatenate([jnp.where(here, code, 0.0) for code in codes], axis=0)
        total = total + lax.dot_general(
            lhs.astype(BF16), hot, (((1,), (1,)), ((), ())), preferred_element_type=F32
        )
    total = total.astype(jnp.int32)
    return total[0:rows], total[rows : 2 * rows] + 256 * total[2 * rows : 3 * rows], count


def split3(value):
    hi = value.astype(BF16).astype(F32)
    rest = value - hi
    mid = rest.astype(BF16).astype(F32)
    return hi, mid, rest - mid


def node_side(node):
    row = iota((8, BLK), 0)
    full = jnp.concatenate([node, jnp.ones((2, BLK), F32)], axis=0)
    ahead = pltpu.roll(full, 3, 0) + time_step * full
    base = jnp.where((row >= 3) & (row < 6), ahead, full)
    place = jnp.where(row < 3, full, 0.0)
    square = split3(ALPHA * jnp.sum(place * place, axis=0, keepdims=True))
    tail = jnp.where(row == 0, square[0], jnp.where(row == 1, square[1], square[2]))
    tail = jnp.where(row < 3, tail, 0.0)
    hi, mid, lo = split3(base)
    rows = jnp.concatenate([hi, mid, lo, hi, mid, hi, tail, jnp.zeros((8, BLK), F32)], axis=0)
    return rows.T.astype(BF16)


def pair_force(geo, node):
    row = iota((8, BLK), 0)
    hi, mid, lo = split3(geo)
    is_e = (row < 3) | (row == 6)
    pieces = [hi, hi, hi, mid, mid, lo]
    left = {id(p): jnp.where(is_e, p, 0.0) for p in (hi, mid, lo)}
    right = {id(p): jnp.where(is_e, 0.0, p) for p in (hi, mid, lo)}
    ones = [jnp.ones((8, BLK), F32)] * 2
    zeros = [jnp.zeros((8, BLK), F32)] * 2
    operand = jnp.concatenate(
        [
            jnp.concatenate([left[id(p)] for p in pieces] + ones, axis=0).astype(BF16),
            jnp.concatenate([right[id(p)] for p in pieces] + zeros, axis=0).astype(BF16),
        ],
        axis=1,
    )
    both = jnp.dot(node, operand, preferred_element_type=F32)
    pressure = jnp.exp2(both[:, 0:BLK]) * jnp.maximum(both[:, BLK:], 0.0)
    top = pressure.astype(BF16)
    bottom = (pressure - top.astype(F32)).astype(BF16)
    weights = jnp.concatenate([hi, mid], axis=0).astype(BF16)
    result = lax.dot_general(
        jnp.concatenate([weights, weights], axis=1),
        jnp.concatenate([top, bottom], axis=1),
        (((1,), (1,)), ((), ())),
        preferred_element_type=F32,
    )
    return result[0:8] + result[8:16]


def force_kernel(
    dom_count, capacity, width, geo_ref, node_ref, dest_ref, out_ref, list_vmem, list_smem, acc_ref, sem
):
    my_dom = lax.axis_index("dom")
    my_row = lax.axis_index("grp")
    devices, planes = geo_ref.shape[0], geo_ref.shape[1]
    seg_blocks = planes - 1
    rows = devices * width // BLK
    tables = []
    for row in range(2):
        full = geo_ref[:, seg_blocks, row, :]
        value = None
        for r in range(BLK // width):
            piece = full[:, r * width : (r + 1) * width]
            value = piece if value is None else jnp.where(my_row == r, piece, value)
        tables.append(pack_lanes(value, rows).astype(jnp.int32))
    nodes, blocks, count = pair_list(
        tables[0], tables[1], dest_ref[...], my_dom, dom_count, seg_blocks, capacity, width
    )
    list_vmem[0:rows] = nodes
    list_vmem[rows : 2 * rows] = blocks
    list_vmem[2 * rows : 2 * rows + 1] = jnp.full((1, BLK), count, F32).astype(jnp.int32)
    copy = pltpu.make_async_copy(list_vmem, list_smem, sem)
    copy.start()
    acc_ref[...] = jnp.zeros_like(acc_ref)
    copy.wait()
    pairs = list_smem[2 * rows, 0]

    def body(step, carry):
        results = []
        for u in range(UNROLL):
            p = jnp.minimum(step * UNROLL + u, rows * BLK - 1)
            node_id = list_smem[p // BLK, p % BLK]
            block_id = list_smem[rows + p // BLK, p % BLK]
            geo = geo_ref[block_id // seg_blocks, block_id % seg_blocks]
            results.append((p, node_id, pair_force(geo, node_ref[node_id])))
        for u in range(UNROLL):
            p, node_id, force = results[u]
            scale = jnp.where(step * UNROLL + u < pairs, -1.0 / stiffness, 0.0)
            acc_ref[node_id] = acc_ref[node_id] + scale * force
        return carry

    lax.fori_loop(0, (pairs + UNROLL - 1) // UNROLL, body, 0)
    for axis in range(3):
        out_ref[axis] = acc_ref[:, 3 + axis, :]


def shards(node_state, node_dest, seg_nodes, seg_conn, pair_seg, pair_slot):
    dom_count = lax.axis_size("dom")
    grp_count = lax.axis_size("grp")
    devices = dom_count * grp_count
    block_count = node_state.shape[0]
    capacity = max(2, 2 * block_count // dom_count)
    width = pair_seg.shape[2]
    seg_blocks = seg_conn.shape[1] // BLK
    rows = devices * width // BLK
    vmem_limit = 24 * 2**20
    gathered, left, dest = pl.pallas_call(
        functools.partial(gather_kernel, grp_count, dom_count),
        out_shape=(
            pltpu.VMEM((devices, seg_blocks + 1, 8, BLK), F32),
            pltpu.VMEM((block_count, BLK, 64), BF16),
            pltpu.VMEM((1, block_count), jnp.int32),
        ),
        in_specs=[pl.BlockSpec(memory_space=pltpu.HBM)] * 6,
        out_specs=(VMEM, VMEM, VMEM),
        scratch_shapes=[
            pltpu.VMEM(seg_nodes.shape, F32),
            pltpu.VMEM(seg_conn.shape, jnp.int32),
            pltpu.VMEM(pair_seg.shape, jnp.int32),
            pltpu.VMEM(pair_slot.shape, jnp.int32),
            pltpu.VMEM((6, block_count, BLK), F32),
            pltpu.SemaphoreType.DMA((6,)),
            pltpu.SemaphoreType.DMA((dom_count // 2,)),
            pltpu.SemaphoreType.DMA((dom_count // 2 * (grp_count - 1),)),
            pltpu.SemaphoreType.DMA((devices,)),
            pltpu.SemaphoreType.DMA((devices,)),
        ],
        compiler_params=pltpu.CompilerParams(collective_id=0, has_side_effects=True, vmem_limit_bytes=vmem_limit),
    )(
        *(
            pltpu.with_memory_space_constraint(x, pltpu.HBM)
            for x in (
                seg_nodes,
                seg_conn,
                pair_seg,
                pair_slot,
                jnp.transpose(node_state, (1, 0, 2)),
                node_dest.reshape(1, block_count),
            )
        )
    )
    force = pl.pallas_call(
        functools.partial(force_kernel, dom_count, capacity, width),
        out_shape=jax.ShapeDtypeStruct((3, block_count, BLK), F32),
        in_specs=[VMEM] * 3,
        out_specs=VMEM,
        scratch_shapes=[
            pltpu.VMEM((2 * rows + 8, BLK), jnp.int32),
            pltpu.SMEM((2 * rows + 8, BLK), jnp.int32),
            pltpu.VMEM((block_count, 8, BLK), F32),
            pltpu.SemaphoreType.DMA,
        ],
        compiler_params=pltpu.CompilerParams(vmem_limit_bytes=vmem_limit),
    )(
        pltpu.with_memory_space_constraint(gathered, pltpu.VMEM),
        pltpu.with_memory_space_constraint(left, pltpu.VMEM),
        pltpu.with_memory_space_constraint(dest, pltpu.VMEM),
    )
    return jnp.transpose(force, (1, 0, 2))


def solution(mesh):
    in_specs = (
        P(("grp", "dom"), None, None),
        P(("grp", "dom")),
        P(None, ("grp", "dom")),
        P(None, ("grp", "dom")),
        P(("grp", "dom"), None, None),
        P(("grp", "dom"), None, None),
    )
    out_specs = P(("grp", "dom"), None, None)
    return jax.shard_map(shards, mesh=mesh, in_specs=in_specs, out_specs=out_specs, check_vma=False)
```
